128 devices in a mesh: rep: 1, dp: 128 (over x, y, z, core).
Axes of the slice: x: 4, y: 4, z: 4, core: 2. Of those that a mesh axis runs over, the one named last changes fastest.
Arguments:
- g_w_gate: bfloat16 [128, 2, 512, 8192], P(('rep', 'dp'))
- g_w_up: bfloat16 [128, 2, 512, 8192], P(('rep', 'dp'))
- g_w_down: bfloat16 [128, 2, 8192, 512], P(('rep', 'dp'))
- w_gate: bfloat16 [2, 512, 8192], replicated
- w_up: bfloat16 [2, 512, 8192], replicated
- w_down: bfloat16 [2, 8192, 512], replicated
- m_w_gate: float32 [2, 512, 8192], P(None, 'dp')
- m_w_up: float32 [2, 512, 8192], P(None, 'dp')
- m_w_down: float32 [2, 8192, 512], P(None, 'dp')
- v_w_gate: float32 [2, 512, 8192], P(None, 'dp')
- v_w_up: float32 [2, 512, 8192], P(None, 'dp')
- v_w_down: float32 [2, 8192, 512], P(None, 'dp')
Outputs:
- output 1: bfloat16 [2, 512, 8192], P('rep')
- output 2: bfloat16 [2, 512, 8192], P('rep')
- output 3: bfloat16 [2, 8192, 512], P('rep')
- output 4: float32 [2, 512, 8192], P('rep', 'dp')
- output 5: float32 [2, 512, 8192], P('rep', 'dp')
- output 6: float32 [2, 8192, 512], P('rep', 'dp')
- output 7: float32 [2, 512, 8192], P('rep', 'dp')
- output 8: float32 [2, 512, 8192], P('rep', 'dp')
- output 9: float32 [2, 8192, 512], P('rep', 'dp')
All inputs are finite; a program needn't handle non-finite values.
Results may differ from the reference program's by a relative error of at most 0.022.
Values are sent between devices in bfloat16 or wider.
A program may use at most 1.5 GiB of HBM per device.

```python
import jax
import jax.numpy as jnp
from jax import lax

DEVICES = 128
D = 512
FF = 8192
LAYERS = 2
NAMES = ("w_gate", "w_up", "w_down")
SHAPES = {"w_gate": (LAYERS, D, FF), "w_up": (LAYERS, D, FF), "w_down": (LAYERS, FF, D)}


def setup_inputs(seed: int = 0, part: int = 0) -> dict:
    kz, *keys = jax.random.split(jax.random.key(seed), 1 + 5 * len(NAMES))
    loud = 2.0 ** jax.random.uniform(kz, (), jnp.float32, -1.0, 1.0)
    drawn = {}
    for name, key, both in zip(NAMES, keys[:3], keys[3:6], strict=True):
        own = jax.random.normal(jax.random.fold_in(key, part), (DEVICES, *SHAPES[name]), jnp.float32)
        shared = jax.random.normal(jax.random.fold_in(both, part), SHAPES[name], jnp.float32)
        drawn["g_" + name] = (loud * (0.7 * shared / DEVICES + 0.7 * own * DEVICES**-0.5)).astype(jnp.bfloat16)
    for name, key in zip(NAMES, keys[6:9], strict=True):
        drawn[name] = (jax.random.normal(key, SHAPES[name], jnp.float32) * SHAPES[name][1] ** -0.5).astype(jnp.bfloat16)
    for name, key in zip(NAMES, keys[9:12], strict=True):
        drawn["m_" + name] = loud * 0.5 * jax.random.normal(key, SHAPES[name], jnp.float32)
    for name, key in zip(NAMES, keys[12:15], strict=True):
        drawn["v_" + name] = loud * loud * jax.random.uniform(key, SHAPES[name], jnp.float32, 0.5, 1.5)
    return drawn


def adamw(w, m, v, g):
    m = 0.9 * m + 0.1 * g
    v = 0.95 * v + 0.05 * g * g
    step = m * lax.rsqrt(v + 1e-8) + 0.1 * w
    return (w - 0.02 * step).astype(jnp.bfloat16), m, v


def clipped(gradients, sum_of_squares, count):
    factor = jnp.minimum(1.0, 0.5 * lax.rsqrt(sum_of_squares / count + 1e-30))
    return [g * factor for g in gradients]


def reference(g_w_gate, g_w_up, g_w_down, w_gate, w_up, w_down, m_w_gate, m_w_up, m_w_down, v_w_gate, v_w_up, v_w_down):
    def total(terms):
        return lax.scan(lambda so_far, term: (so_far + term.astype(jnp.float32), None), jnp.zeros(terms.shape[1:], jnp.float32), terms)[0]

    gradients = [total(terms).astype(jnp.bfloat16).astype(jnp.float32) for terms in (g_w_gate, g_w_up, g_w_down)]
    gradients = clipped(gradients, sum(jnp.sum(g * g) for g in gradients), sum(g.size for g in gradients))
    new = [
        adamw(w.astype(jnp.float32), m, v, g)
        for w, m, v, g in zip((w_gate, w_up, w_down), (m_w_gate, m_w_up, m_w_down), (v_w_gate, v_w_up, v_w_down), gradients, strict=True)
    ]
    return tuple(one[which] for which in range(3) for one in new)
```

```python
import functools

import jax
import jax.numpy as jnp
from jax import lax
from jax.experimental import pallas as pl
from jax.experimental.pallas import tpu as pltpu
from jax.sharding import PartitionSpec as P

N = 4
DEVICES = 2 * N**3
ORDERS = ((0, 1, 2), (1, 2, 0), (2, 0, 1))
COLORS = tuple((which, layer) for which in range(3) for layer in range(2))
F32, BF16 = jnp.float32, jnp.bfloat16


def place():
    me = lax.axis_index("dp")
    chip = me // 2
    return lax.rem(me, 2), (chip // (N * N), lax.rem(chip // N, N), lax.rem(chip, N))


def device(core, chip):
    return {"dp": ((chip[0] * N + chip[1]) * N + chip[2]) * 2 + core}


def moved(chip, axis, by):
    return tuple(lax.rem(c + by + N, N) if a == axis else c for a, c in enumerate(chip))


def along(color, chip):
    which, layer = color
    axes = ORDERS[which]
    return axes, 1 - 2 * layer, tuple(chip[a] for a in axes)


def back(c, s, by):
    return lax.rem(c - s * by + N, N)


def block(ref, color, abc, tiles):
    axes = ORDERS[color[0]]
    where = [slice(None)] * 3
    for a, c in zip(axes, abc, strict=True):
        if c is not None:
            where[a] = c
    return ref.at[(color[1], *where, tiles)]


def send(src, dst, send_sem, recv_sem, to):
    copy = pltpu.make_async_remote_copy(
        src_ref=src, dst_ref=dst, send_sem=send_sem, recv_sem=recv_sem, device_id=to, device_id_type=pl.DeviceIdType.MESH
    )
    copy.start()
    return copy


def arrived(ref, sem):
    pltpu.make_async_copy(ref, ref, sem).wait()


def meet(peers):
    barrier = pltpu.get_barrier_semaphore()
    for peer in peers:
        pl.semaphore_signal(barrier, inc=1, device_id=peer, device_id_type=pl.DeviceIdType.MESH)
    pl.semaphore_wait(barrier, len(peers))


def add_up(out, ins, step):
    @pl.loop(0, out.shape[0] // step)
    def _(n):
        at = pl.ds(n * step, step)
        total = ins[0][at].astype(F32)
        for one in ins[1:]:
            total = total + one[at].astype(F32)
        out[at] = total.astype(out.dtype)


def scatter_kernel(
    g0, g1, g2, w0, w1, w2, m_wide, m_tall, v_wide, v_tall,
    w_out, g_wide, g_tall, factor_out,
    own, par, r1, r2, r3, g_send, w_chip, w_chip_tall, w_rows, w_got, norm, norm_got, mom,
    own_sem, par_send, par_recv, send1, recv1, send2, recv2, send3, recv3,
    norm_send, norm_recv, swap_send, swap_recv, back_send, back_recv, load_sem,
):
    g, w = (g0, g1, g2), (w0, w1, w2)
    core, chip = place()
    half = w_out.shape[1]
    step = min(8, half)
    mine, theirs = pl.ds(core * half, half), pl.ds((1 - core) * half, half)
    partner = device(1 - core, chip)
    meet([partner] + [device(core, moved(chip, axis, by)) for axis in range(3) for by in range(1, N)])

    def targets(color, t, k):
        axes, s, (a, b, c) = along(color, chip)
        return back(a, s, t + 1), back(b, s, k + 1), None

    def own_copy(n, t, k):
        return pltpu.make_async_copy(block(g[COLORS[n][0]], COLORS[n], targets(COLORS[n], t, k), mine), own.at[k, n], own_sem.at[k, n])

    def push(n, t, k):
        own_copy(n, t, k).start()
        src = block(g[COLORS[n][0]], COLORS[n], targets(COLORS[n], t, k), theirs)
        send(src, par.at[n, t, k], par_send.at[n, t, k], par_recv.at[n, t, k], partner)

    @pl.loop(0, N)
    def _(k):
        for n in range(6):
            push(n, 0, k)

    loads = []
    for n, (which, layer) in enumerate(COLORS):
        if which < 2:
            loads.append((block(w[which], COLORS[n], along(COLORS[n], chip)[2], slice(None)), w_chip.at[n]))
        else:
            loads.append((block(w[which], COLORS[n], along(COLORS[n], chip)[2], mine), w_chip_tall.at[layer]))
    loads = [pltpu.make_async_copy(src, dst, load_sem.at[i]) for i, (src, dst) in enumerate(loads)]
    for load in loads:
        load.start()

    def flat(ref):
        return [ref.at[q] for q in range(N)]

    def ready(n, t, k):
        own_copy(n, t, k).wait()
        arrived(par.at[n, t, k], par_recv.at[n, t, k])

    def along_a(n, t, k, first):
        axes, s, _ = along(COLORS[n], chip)
        ready(n, t, k)
        ins = [own.at[k, n], par.at[n, t, k]]
        if not first:
            arrived(r1.at[n, t - 1, k], recv1.at[n, t - 1, k])
            ins.append(r1.at[n, t - 1, k])

        @pl.loop(0, N)
        def _(q):
            add_up(par.at[n, t, k, q], [one.at[q] for one in ins], step)

        send(par.at[n, t, k], r1.at[n, t, k], send1.at[n, t, k], recv1.at[n, t, k], device(core, moved(chip, axes[0], s)))
        push(n, t + 1, k)

    @pl.loop(0, N)
    def _(k):
        for n in range(6):
            along_a(n, 0, k, True)

    @pl.loop(0, 2 * N)
    def _(i):
        for n in range(6):
            along_a(n, 1 + i // N, lax.rem(i, N), False)

    def along_b(n, k, j, first):
        axes, s, (a, b, c) = along(COLORS[n], chip)
        to = back(c, s, j + 1)
        ins = [own.at[k, n, to], par.at[n, N - 1, k, to], r1.at[n, N - 2, k, to]]
        if not first:
            arrived(r2.at[n, k - 1, to], recv2.at[n, k - 1, j])
            ins.append(r2.at[n, k - 1, to])
        out = par.at[n, N - 1, k, to]
        add_up(out, ins, step)
        send(out, r2.at[n, k, to], send2.at[n, k, j], recv2.at[n, k, j], device(core, moved(chip, axes[1], s)))

    def phase_b(k, first):
        for n in range(6):
            ready(n, N - 1, k)
            arrived(r1.at[n, N - 2, k], recv1.at[n, N - 2, k])

        @pl.loop(0, N)
        def _(j):
            for n in range(6):
                along_b(n, k, j, first)

    phase_b(0, True)

    @pl.loop(1, N - 1)
    def _(k):
        phase_b(k, False)

    def parts_c(n, j, first):
        axes, s, (a, b, c) = along(COLORS[n], chip)
        k = N - 1
        to = back(c, s, j + 1)
        arrived(r2.at[n, k - 1, to], recv2.at[n, k - 1, j])
        ins = [own.at[k, n, to], par.at[n, N - 1, k, to], r1.at[n, N - 2, k, to], r2.at[n, k - 1, to]]
        if not first:
            arrived(r3.at[n, j - 1], recv3.at[n, j - 1])
            ins.append(r3.at[n, j - 1])
        return par.at[n, N - 1, k, to], ins

    def along_c(n, j, first):
        axes, s, _ = along(COLORS[n], chip)
        out, ins = parts_c(n, j, first)
        add_up(out, ins, step)
        send(out, r3.at[n, j], send3.at[n, j], recv3.at[n, j], device(core, moved(chip, axes[2], s)))

    for n in range(6):
        ready(n, N - 1, N - 1)
        arrived(r1.at[n, N - 2, N - 1], recv1.at[n, N - 2, N - 1])
        along_c(n, 0, True)

    @pl.loop(1, N - 1)
    def _(j):
        for n in range(6):
            along_c(n, j, False)

    norm[0] = jnp.zeros(norm.shape[1:], F32)
    for n, (which, layer) in enumerate(COLORS):
        _, ins = parts_c(n, N - 1, False)

        @pl.loop(0, half // step, init_carry=jnp.zeros(norm.shape[1:], F32))
        def squares(i, so_far, ins=ins, which=which, layer=layer, n=n):
            at = pl.ds(i * step, step)
            total = ins[0][at].astype(F32)
            for one in ins[1:]:
                total = total + one[at].astype(F32)
            rounded = total.astype(BF16)
            total = rounded.astype(F32)
            if which < 2:
                low, high = total[:, :4], total[:, 4:]
                g_wide[n, pl.ds(core * half + i * step, step)] = jnp.where(core == 0, low, high).astype(BF16)
                g_send[n, at] = jnp.where(core == 0, high, low).astype(BF16)
            else:
                g_tall[layer, at] = rounded
            return so_far + jnp.sum(total * total, axis=0)

        norm[0] += squares
        if which < 2:
            send(g_send.at[n], g_wide.at[n, mine], swap_send.at[n], swap_recv.at[n], partner)

    send(norm.at[0], norm_got.at[0, 0], norm_send.at[0, 0], norm_recv.at[0, 0], partner)
    arrived(norm_got.at[0, 0], norm_recv.at[0, 0])
    norm[1] = norm[0] + norm_got[0, 0]
    for axis in range(3):
        for d in range(1, N):
            send(
                norm.at[1 + axis], norm_got.at[1 + axis, d - 1], norm_send.at[1 + axis, d - 1], norm_recv.at[1 + axis, d - 1],
                device(core, moved(chip, axis, d)),
            )
        total = norm[1 + axis]
        for d in range(1, N):
            arrived(norm_got.at[1 + axis, d - 1], norm_recv.at[1 + axis, d - 1])
            total = total + norm_got[1 + axis, d - 1]
        norm[2 + axis] = total
    count = 6 * N**3 * 2 * half * 8 * 128
    everything = jnp.sum(norm[4], keepdims=True)
    factor = jnp.minimum(1.0, 0.5 * lax.rsqrt(everything / count + 1e-30))
    factor_out[...] = jnp.broadcast_to(factor, factor_out.shape)

    for load in loads:
        load.wait()
    for n in range(4):
        arrived(g_wide.at[n, theirs], swap_recv.at[n])

    def new_weight(old, m, v, grad):
        m = 0.9 * m + 0.1 * grad
        v = 0.95 * v + 0.05 * grad * grad
        return (old - 0.02 * (m * lax.rsqrt(v + 1e-8) + 0.1 * old)).astype(BF16)

    for n in range(4):

        @pl.loop(0, 2 * half // step)
        def _(i, n=n):
            at = pl.ds(i * step, step)
            old = w_chip[n, at].astype(F32)
            old = jnp.where(core == 0, old[:, :4], old[:, 4:])
            scale = jnp.broadcast_to(factor[:, :, None], old.shape)
            w_rows[n, at] = new_weight(old, m_wide[n, at], v_wide[n, at], g_wide[n, at].astype(F32) * scale)

        send(w_rows.at[n, theirs], w_got.at[n], back_send.at[n], back_recv.at[n], partner)

    for layer in range(2):

        @pl.loop(0, half // step)
        def _(i, layer=layer):
            at = pl.ds(i * step, step)
            old = w_chip_tall[layer, at].astype(F32)
            scale = jnp.broadcast_to(factor[:, :, None], old.shape)
            w_out[4 + layer, at] = new_weight(old, m_tall[layer, at], v_tall[layer, at], g_tall[layer, at].astype(F32) * scale)

    for n in range(4):
        arrived(w_got.at[n], back_recv.at[n])

        @pl.loop(0, half // step)
        def _(i, n=n):
            at = pl.ds(i * step, step)
            kept = w_rows[n, pl.ds(core * half + i * step, step)].astype(F32)
            got = w_got[n, at].astype(F32)
            low, high = jnp.where(core == 0, kept, got), jnp.where(core == 0, got, kept)
            w_out[n, at] = jnp.concatenate([low, high], axis=1).astype(BF16)

    @pl.loop(0, N * N)
    def _(i):
        t, k = i // N, lax.rem(i, N)
        for n in range(6):
            arrived(par.at[n, t, k], par_send.at[n, t, k])

    @pl.loop(0, (N - 1) * N)
    def _(i):
        t, k = i // N, lax.rem(i, N)
        for n in range(6):
            arrived(r1.at[n, t, k], send1.at[n, t, k])
            arrived(r2.at[n, t, k], send2.at[n, t, k])

    for n in range(6):
        for j in range(N - 1):
            arrived(r3.at[n, j], send3.at[n, j])
    for n in range(4):
        arrived(g_send.at[n], swap_send.at[n])
        arrived(w_got.at[n], back_send.at[n])
    arrived(norm.at[0], norm_send.at[0, 0])
    for axis in range(3):
        for d in range(1, N):
            arrived(norm.at[0], norm_send.at[1 + axis, d - 1])


def scatter(g, w, m, v, tiles):
    half = tiles // 2
    any_, vmem = pl.BlockSpec(memory_space=pltpu.HBM), pl.BlockSpec(memory_space=pltpu.VMEM)
    dma = pltpu.SemaphoreType.DMA
    chunk = (N, half, 8, 128)
    return pl.pallas_call(
        scatter_kernel,
        out_shape=[
            jax.ShapeDtypeStruct((6, half, 8, 128), BF16),
            jax.ShapeDtypeStruct((4, tiles, 4, 128), BF16),
            jax.ShapeDtypeStruct((2, half, 8, 128), BF16),
            jax.ShapeDtypeStruct((8, 128), F32),
        ],
        in_specs=[any_] * 6 + [vmem] * 4,
        out_specs=[vmem] * 4,
        scratch_shapes=[
            pltpu.VMEM((N, 6, *chunk), BF16),
            pltpu.VMEM((6, N, N, *chunk), BF16),
            pltpu.VMEM((6, N - 1, N, *chunk), BF16),
            pltpu.VMEM((6, N - 1, *chunk), BF16),
            pltpu.VMEM((6, N - 1, half, 8, 128), BF16),
            pltpu.VMEM((4, half, 4, 128), BF16),
            pltpu.VMEM((4, tiles, 8, 128), BF16),
            pltpu.VMEM((2, half, 8, 128), BF16),
            pltpu.VMEM((4, tiles, 4, 128), BF16),
            pltpu.VMEM((4, half, 4, 128), BF16),
            pltpu.VMEM((5, 8, 128), F32),
            pltpu.VMEM((4, N - 1, 8, 128), F32),
            pltpu.VMEM((8, 128), F32),
            dma((N, 6)),
            dma((6, N, N)),
            dma((6, N, N)),
            dma((6, N - 1, N)),
            dma((6, N - 1, N)),
            dma((6, N - 1, N)),
            dma((6, N - 1, N)),
            dma((6, N - 1)),
            dma((6, N - 1)),
            dma((4, N - 1)),
            dma((4, N - 1)),
            dma((4,)),
            dma((4,)),
            dma((4,)),
            dma((4,)),
            dma((6,)),
        ],
        compiler_params=pltpu.CompilerParams(collective_id=0, has_side_effects=True, vmem_limit_bytes=67043328),
        name="scatter",
    )(*g, *w, m[0], m[1], v[0], v[1])


def gather_kernel(own, w0, w1, w2, local_sem, send_c, recv_c, send_b, recv_b, send_a, recv_a, send_p, recv_p):
    w = (w0, w1, w2)
    core, chip = place()
    half = own.shape[1]
    mine, theirs = pl.ds(core * half, half), pl.ds((1 - core) * half, half)
    partner = device(1 - core, chip)
    meet([partner] + [device(core, moved(chip, axis, by)) for axis in range(3) for by in (1, N - 1)])

    def at(n, i, j, k, tiles=mine):
        _, s, (a, b, c) = along(COLORS[n], chip)
        return block(w[COLORS[n][0]], COLORS[n], (back(a, s, i), back(b, s, j), None if k is None else back(c, s, k)), tiles)

    def to(n, phase):
        axes, s, _ = along(COLORS[n], chip)
        return device(core, moved(chip, axes[phase], s))

    for n in range(6):
        pltpu.make_async_copy(own.at[n], at(n, 0, 0, 0), local_sem.at[n]).start()
        send(own.at[n], at(n, 0, 0, 0), send_c.at[n, 0], recv_c.at[n, 0], to(n, 2))
        send(own.at[n], at(n, 0, 0, 0), send_b.at[n, 0, 0], recv_b.at[n, 0, 0], to(n, 1))
        send(own.at[n], at(n, 0, 0, 0), send_a.at[n, 0, 0, 0], recv_a.at[n, 0, 0, 0], to(n, 0))
        send(own.at[n], at(n, 0, 0, 0), send_p.at[n, 0, 0, 0], recv_p.at[n, 0, 0, 0], partner)

    def pass_on(n, i, j, k):
        here = at(n, i, j, k)
        send(here, here, send_a.at[n, i, j, k], recv_a.at[n, i, j, k], to(n, 0))
        send(here, here, send_p.at[n, i, j, k], recv_p.at[n, i, j, k], partner)

    def row(k):
        for n in range(6):
            here = at(n, 0, 0, k)
            arrived(here, recv_c.at[n, k - 1])

            @pl.when(k < N - 1)
            def _(n=n, here=here):
                send(here, here, send_c.at[n, k], recv_c.at[n, k], to(n, 2))

            send(here, here, send_b.at[n, 0, k], recv_b.at[n, 0, k], to(n, 1))
            pass_on(n, 0, 0, k)

    def plane(j, k):
        for n in range(6):
            here = at(n, 0, j, k)
            arrived(here, recv_b.at[n, j - 1, k])

            @pl.when(j < N - 1)
            def _(n=n, here=here):
                send(here, here, send_b.at[n, j, k], recv_b.at[n, j, k], to(n, 1))

            pass_on(n, 0, j, k)

    @pl.loop(1, 2 * N - 1)
    def _(far):
        @pl.loop(0, N)
        def _(j):
            k = far - j

            @pl.when((j == 0) & (k < N))
            def _():
                row(k)

            @pl.when((j > 0) & (k >= 0) & (k < N))
            def _():
                plane(j, k)

    def beyond(i, last):
        @pl.loop(0, N * N)
        def _(x):
            j, k = x // N, lax.rem(x, N)
            for n in range(6):
                here = at(n, i, j, k)
                arrived(here, recv_a.at[n, i - 1, j, k])
                if not last:
                    send(here, here, send_a.at[n, i, j, k], recv_a.at[n, i, j, k], to(n, 0))
                send(here, here, send_p.at[n, i, j, k], recv_p.at[n, i, j, k], partner)

    @pl.loop(1, N - 1)
    def _(i):
        beyond(i, False)

    beyond(N - 1, True)

    for n in range(6):
        here = at(n, 0, 0, 0)
        pltpu.make_async_copy(own.at[n], here, local_sem.at[n]).wait()
        for k in range(N - 1):
            arrived(here, send_c.at[n, k])

    @pl.loop(0, N * N)
    def _(x):
        j, k = x // N, lax.rem(x, N)
        for n in range(6):
            here = at(n, 0, j, k)

            @pl.when(j < N - 1)
            def _(n=n, here=here):
                arrived(here, send_b.at[n, j, k])

            for i in range(N):
                if i < N - 1:
                    arrived(here, send_a.at[n, i, j, k])
                arrived(here, send_p.at[n, i, j, k])
                arrived(at(n, i, j, k, theirs), recv_p.at[n, i, j, k])


def gather(own, tiles):
    any_, vmem = pl.BlockSpec(memory_space=pltpu.HBM), pl.BlockSpec(memory_space=pltpu.VMEM)
    dma = pltpu.SemaphoreType.DMA
    return pl.pallas_call(
        gather_kernel,
        out_shape=[jax.ShapeDtypeStruct((2, N, N, N, tiles, 8, 128), BF16)] * 3,
        in_specs=[vmem],
        out_specs=[any_] * 3,
        scratch_shapes=[
            dma((6,)),
            dma((6, N - 1)),
            dma((6, N - 1)),
            dma((6, N - 1, N)),
            dma((6, N - 1, N)),
            dma((6, N - 1, N, N)),
            dma((6, N - 1, N, N)),
            dma((6, N, N, N)),
            dma((6, N, N, N)),
        ],
        compiler_params=pltpu.CompilerParams(collective_id=1, has_side_effects=True),
        name="gather",
    )(own)


def wide_tiles(t, *major):
    rows = t.shape[-2] // functools.reduce(lambda a, b: a * b, major, 1)
    lead = t.shape[:-2]
    t = t.reshape(*lead, *major, rows, t.shape[-1] // 128, 128)
    return jnp.swapaxes(t, -3, -2)


def tall_tiles(t, *major):
    rows = t.shape[-2] // functools.reduce(lambda a, b: a * b, major, 1)
    lead = t.shape[:-2]
    t = t.reshape(*lead, *major, rows // 8, 8, t.shape[-1] // 128, 128)
    t = jnp.swapaxes(t, -3, -2)
    return t.reshape(*lead, *major, -1, 8, 128)


def from_wide(t, shape):
    return jnp.swapaxes(t, -3, -2).reshape(shape)


def from_tall(t, shape):
    columns = shape[-1] // 128
    t = t.reshape(*t.shape[:-3], t.shape[-3] // columns, columns, 8, 128)
    return jnp.swapaxes(t, -3, -2).reshape(shape)


def solution(mesh):
    def step(*arrays):
        terms, weights, m, v = (arrays[i : i + 3] for i in (0, 3, 6, 9))
        g = [wide_tiles(terms[0][0], N, N, N), wide_tiles(terms[1][0], N, N, N), tall_tiles(terms[2][0], N, N, N)]
        w = [wide_tiles(weights[0], N, N, N), wide_tiles(weights[1], N, N, N), tall_tiles(weights[2], N, N, N)]
        tiles = g[0].shape[4]

        def moments(one):
            return jnp.concatenate([wide_tiles(one[0]), wide_tiles(one[1])]), tall_tiles(one[2])

        own, g_wide, g_tall, factor = scatter(g, w, moments(m), moments(v), tiles)
        whole = gather(own, tiles)
        whole = [from_wide(whole[0], weights[0].shape), from_wide(whole[1], weights[1].shape), from_tall(whole[2], weights[2].shape)]
        grads = [from_wide(g_wide[:2], m[0].shape), from_wide(g_wide[2:], m[1].shape), from_tall(g_tall, m[2].shape)]
        grads = [one.astype(F32) * factor[0, 0] for one in grads]
        new_m = [0.9 * one + 0.1 * grad for one, grad in zip(m, grads, strict=True)]
        new_v = [0.95 * one + 0.05 * grad * grad for one, grad in zip(v, grads, strict=True)]
        return (*whole, *new_m, *new_v)

    all_of, cut = P(None, None, None), P(None, "dp", None)
    return jax.shard_map(
        step,
        mesh=mesh,
        in_specs=(P(("rep", "dp"), None, None, None),) * 3 + (all_of,) * 3 + (cut,) * 6,
        out_specs=(P("rep", None, None),) * 3 + (P("rep", "dp", None),) * 6,
        check_vma=False,
    )
```

```python
import functools

import jax
import jax.numpy as jnp
from jax import lax
from jax.experimental import pallas as pl
from jax.experimental.pallas import tpu as pltpu
from jax.sharding import PartitionSpec as P

N = 4
AHEAD = 3
STEP = 8
STEP_LIMIT, FINISH_LIMIT = 10 * 2**20, 4 * 2**20
DEVICES = 2 * N**3
ORDERS = ((0, 1, 2), (1, 2, 0), (2, 0, 1))
COLORS = tuple((which, layer) for which in range(3) for layer in range(2))
F32, BF16 = jnp.float32, jnp.bfloat16


def place():
    me = lax.axis_index("dp")
    chip = me // 2
    return lax.rem(me, 2), (chip // (N * N), lax.rem(chip // N, N), lax.rem(chip, N))


def device(core, chip):
    return {"dp": ((chip[0] * N + chip[1]) * N + chip[2]) * 2 + core}


def moved(chip, axis, by):
    return tuple(lax.rem(c + by + N, N) if a == axis else c for a, c in enumerate(chip))


def along(color, chip):
    which, layer = color
    axes = ORDERS[which]
    return axes, 1 - 2 * layer, tuple(chip[a] for a in axes)


def back(c, s, by):
    return lax.rem(c - s * by + N, N)


def block(ref, color, abc, tiles):
    axes = ORDERS[color[0]]
    where = [slice(None)] * 3
    for a, c in zip(axes, abc, strict=True):
        if c is not None:
            where[a] = c
    return ref.at[(color[1], *where, tiles)]


def send(src, dst, send_sem, recv_sem, to):
    copy = pltpu.make_async_remote_copy(
        src_ref=src, dst_ref=dst, send_sem=send_sem, recv_sem=recv_sem, device_id=to, device_id_type=pl.DeviceIdType.MESH
    )
    copy.start()
    return copy


def arrived(ref, sem):
    pltpu.make_async_copy(ref, ref, sem).wait()


def meet(peers):
    barrier = pltpu.get_barrier_semaphore()
    for peer in peers:
        pl.semaphore_signal(barrier, inc=1, device_id=peer, device_id_type=pl.DeviceIdType.MESH)
    pl.semaphore_wait(barrier, len(peers))


def add_up(out, ins, step):
    @pl.loop(0, out.shape[0] // step)
    def _(n):
        at = pl.ds(n * step, step)
        total = ins[0][at].astype(F32)
        for one in ins[1:]:
            total = total + one[at].astype(F32)
        out[at] = total.astype(out.dtype)


def step_kernel(
    g0, g1, g2, w0, w1, w2, m0, m1, m2, v0, v1, v2,
    g_wide, g_tall, factor_out, whole,
    own, g_send, w_chip, w_chip_tall, w_rows, w_got, m_wide, m_tall, v_wide, v_tall, norm, norm_got,
    own_sem, par_send, par_recv, send1, recv1, send2, recv2, send3, recv3,
    norm_send, norm_recv, swap_send, swap_recv, back_send, back_recv, load_sem,
    send_c, recv_c, send_b, recv_b, send_a, recv_a, send_p, recv_p,
):
    g, w = (g0, g1, g2), (w0, w1, w2)
    core, chip = place()
    half = own.shape[3]
    step = min(STEP, half)
    mine, theirs = pl.ds(core * half, half), pl.ds((1 - core) * half, half)
    low, high = pl.ds(0, half), pl.ds(half, half)
    partner = device(1 - core, chip)

    def colored(n):
        return whole.at[COLORS[n][0], COLORS[n][1]]

    def par(n, t, k):
        return colored(n).at[t, k, :, low]

    def r1(n, t, k):
        return colored(n).at[t, k, :, high]

    def r2(n, k):
        return colored(n).at[N - 1, k, :, high]

    def r3(n, j):
        return colored(n).at[N - 1, N - 1, j, high]

    def blocks(n, count):
        if count < N:
            return colored(n).at[0, 0, pl.ds(0, count), low]
        if count < N * N:
            return colored(n).at[0, pl.ds(0, count // N), :, low]
        return colored(n).at[pl.ds(0, count // (N * N)), :, :, low]

    def to(n, phase):
        axes, s, _ = along(COLORS[n], chip)
        return device(core, moved(chip, axes[phase], s))

    def targets(color, t, k):
        axes, s, (a, b, c) = along(color, chip)
        return back(a, s, t + 1), back(b, s, k + 1), None

    def own_copy(n, t, k):
        return pltpu.make_async_copy(block(g[COLORS[n][0]], COLORS[n], targets(COLORS[n], t, k), mine), own.at[k, n], own_sem.at[k, n])

    def push(n, t, k):
        src = block(g[COLORS[n][0]], COLORS[n], targets(COLORS[n], t, k), theirs)
        send(src, par(n, t, k), par_send.at[n], par_recv.at[n, t, k], partner)

    @pl.loop(0, N)
    def _(k):
        for n in range(6):
            own_copy(n, 0, k).start()

    meet([partner] + [device(core, moved(chip, axis, by)) for axis in range(3) for by in range(1, N)])

    @pl.loop(0, AHEAD)
    def _(k):
        for n in range(6):
            push(n, 0, k)

    loads = []
    for n, (which, layer) in enumerate(COLORS):
        if which < 2:
            loads.append((block(w[which], COLORS[n], along(COLORS[n], chip)[2], slice(None)), w_chip.at[n]))
        else:
            loads.append((block(w[which], COLORS[n], along(COLORS[n], chip)[2], mine), w_chip_tall.at[layer]))
    loads += [(m0, m_wide.at[pl.ds(0, 2)]), (m1, m_wide.at[pl.ds(2, 2)]), (m2, m_tall)]
    loads += [(v0, v_wide.at[pl.ds(0, 2)]), (v1, v_wide.at[pl.ds(2, 2)]), (v2, v_tall)]
    loads = [pltpu.make_async_copy(src, dst, load_sem.at[i]) for i, (src, dst) in enumerate(loads)]
    for load in loads:
        load.start()

    def ready(n, t, k):
        own_copy(n, t, k).wait()
        arrived(par(n, t, k), par_recv.at[n, t, k])

    def first_axis(n, t, k, first):
        ready(n, t, k)
        ins = [own.at[k, n], par(n, t, k)]
        if not first:
            arrived(r1(n, t - 1, k), recv1.at[n, t - 1, k])
            ins.append(r1(n, t - 1, k))

        @pl.loop(0, N)
        def _(q):
            add_up(par(n, t, k).at[q], [one.at[q] for one in ins], step)

        send(par(n, t, k), r1(n, t, k), send1.at[n], recv1.at[n, t, k], to(n, 0))
        own_copy(n, t + 1, k).start()
        later = t * N + k + AHEAD
        push(n, later // N, lax.rem(later, N))

    @pl.loop(0, N)
    def _(k):
        for n in range(6):
            first_axis(n, 0, k, True)

    @pl.loop(0, 2 * N)
    def _(i):
        for n in range(6):
            first_axis(n, 1 + i // N, lax.rem(i, N), False)

    def second_axis(n, k, j, first):
        _, s, (_, _, c) = along(COLORS[n], chip)
        at = back(c, s, j + 1)
        ins = [own.at[k, n, at], par(n, N - 1, k).at[at], r1(n, N - 2, k).at[at]]
        if not first:
            arrived(r2(n, k - 1).at[at], recv2.at[n, k - 1, j])
            ins.append(r2(n, k - 1).at[at])
        out = par(n, N - 1, k).at[at]
        add_up(out, ins, step)
        send(out, r2(n, k).at[at], send2.at[n], recv2.at[n, k, j], to(n, 1))

    def second_axis_all(k, first):
        for n in range(6):
            @pl.when(k + AHEAD < N)
            def _(n=n):
                push(n, N - 1, k + AHEAD)

        for n in range(6):
            ready(n, N - 1, k)
            arrived(r1(n, N - 2, k), recv1.at[n, N - 2, k])

        @pl.loop(0, N)
        def _(j):
            for n in range(6):
                second_axis(n, k, j, first)

    second_axis_all(0, True)

    @pl.loop(1, N - 1)
    def _(k):
        second_axis_all(k, False)

    def third_axis_parts(n, j, first):
        _, s, (_, _, c) = along(COLORS[n], chip)
        k = N - 1
        at = back(c, s, j + 1)
        arrived(r2(n, k - 1).at[at], recv2.at[n, k - 1, j])
        ins = [own.at[k, n, at], par(n, N - 1, k).at[at], r1(n, N - 2, k).at[at], r2(n, k - 1).at[at]]
        if not first:
            arrived(r3(n, j - 1), recv3.at[n, j - 1])
            ins.append(r3(n, j - 1))
        return par(n, N - 1, k).at[at], ins

    def third_axis(n, j, first):
        out, ins = third_axis_parts(n, j, first)
        add_up(out, ins, step)
        send(out, r3(n, j), send3.at[n], recv3.at[n, j], to(n, 2))

    for n in range(6):
        ready(n, N - 1, N - 1)
        arrived(r1(n, N - 2, N - 1), recv1.at[n, N - 2, N - 1])
        third_axis(n, 0, True)

    @pl.loop(1, N - 1)
    def _(j):
        for n in range(6):
            third_axis(n, j, False)

    norm[0] = jnp.zeros(norm.shape[1:], F32)
    for n, (which, layer) in enumerate(COLORS):
        _, ins = third_axis_parts(n, N - 1, False)

        @pl.loop(0, half // step, init_carry=jnp.zeros(norm.shape[1:], F32))
        def squares(i, so_far, ins=ins, which=which, layer=layer, n=n):
            at = pl.ds(i * step, step)
            total = ins[0][at].astype(F32)
            for one in ins[1:]:
                total = total + one[at].astype(F32)
            rounded = total.astype(BF16)
            total = rounded.astype(F32)
            if which < 2:
                top, bottom = total[:, :4], total[:, 4:]
                g_wide[n, pl.ds(core * half + i * step, step)] = jnp.where(core == 0, top, bottom).astype(BF16)
                g_send[n, at] = jnp.where(core == 0, bottom, top).astype(BF16)
            else:
                g_tall[layer, at] = rounded
            return so_far + jnp.sum(total * total, axis=0)

        norm[0] += squares
        if which < 2:
            send(g_send.at[n], g_wide.at[n, mine], swap_send.at[n], swap_recv.at[n], partner)

    for n in range(6):
        arrived(blocks(n, (N - 1) * N * N), send1.at[n])
        arrived(blocks(n, (N - 1) * N), send2.at[n])
        arrived(blocks(n, N - 1), send3.at[n])

    send(norm.at[0], norm_got.at[0, 0], norm_send.at[0, 0], norm_recv.at[0, 0], partner)
    arrived(norm_got.at[0, 0], norm_recv.at[0, 0])
    norm[1] = norm[0] + norm_got[0, 0]
    for axis in range(3):
        for d in range(1, N):
            send(
                norm.at[1 + axis], norm_got.at[1 + axis, d - 1], norm_send.at[1 + axis, d - 1], norm_recv.at[1 + axis, d - 1],
                device(core, moved(chip, axis, d)),
            )
        if axis == 0:
            for load in loads:
                load.wait()
            for n in range(4):
                arrived(g_wide.at[n, theirs], swap_recv.at[n])
        total = norm[1 + axis]
        for d in range(1, N):
            arrived(norm_got.at[1 + axis, d - 1], norm_recv.at[1 + axis, d - 1])
            total = total + norm_got[1 + axis, d - 1]
        norm[2 + axis] = total
    count = 6 * N**3 * 2 * half * 8 * 128
    everything = jnp.sum(norm[4], keepdims=True)
    factor = jnp.minimum(1.0, 0.5 * lax.rsqrt(everything / count + 1e-30))
    factor_out[...] = jnp.broadcast_to(factor, factor_out.shape)

    def new_weight(old, m, v, grad):
        m = 0.9 * m + 0.1 * grad
        v = 0.95 * v + 0.05 * grad * grad
        return (old - 0.02 * (m * lax.rsqrt(v + 1e-8) + 0.1 * old)).astype(BF16)

    def at(n, i, j, k, tiles=mine):
        _, s, (a, b, c) = along(COLORS[n], chip)
        return block(whole.at[COLORS[n][0]], COLORS[n], (back(a, s, i), back(b, s, j), None if k is None else back(c, s, k)), tiles)

    def along_a(n, here, i, j):
        send(here, here, send_a.at[n], recv_a.at[n, i, j], to(n, 0))

    def along_b(n, here, j, k):
        send(here, here, send_b.at[n], recv_b.at[n, j, k], to(n, 1))

    def along_c(n, here, k):
        send(here, here, send_c.at[n], recv_c.at[n, k], to(n, 2))

    def across(n, here):
        send(here, here, send_p.at[n], recv_p.at[n], partner)

    def start(n):
        here = at(n, 0, 0, 0)
        along_c(n, here, 0)
        along_b(n, here, 0, 0)
        along_a(n, here, 0, 0)

    for n in range(4):

        @pl.loop(0, 2 * half // step)
        def _(i, n=n):
            at = pl.ds(i * step, step)
            old = w_chip[n, at].astype(F32)
            old = jnp.where(core == 0, old[:, :4], old[:, 4:])
            scale = jnp.broadcast_to(factor[:, :, None], old.shape)
            w_rows[n, at] = new_weight(old, m_wide[n, at], v_wide[n, at], g_wide[n, at].astype(F32) * scale)

        send(w_rows.at[n, theirs], w_got.at[n], back_send.at[n], back_recv.at[n], partner)

    for n in (4, 5):
        here = at(n, 0, 0, 0)

        @pl.loop(0, half // step)
        def _(i, layer=n - 4, here=here):
            at = pl.ds(i * step, step)
            old = w_chip_tall[layer, at].astype(F32)
            scale = jnp.broadcast_to(factor[:, :, None], old.shape)
            here[at] = new_weight(old, m_tall[layer, at], v_tall[layer, at], g_tall[layer, at].astype(F32) * scale)

        start(n)

    for n in range(4):
        here = at(n, 0, 0, 0)
        arrived(w_got.at[n], back_recv.at[n])

        @pl.loop(0, half // step)
        def _(i, n=n, here=here):
            at = pl.ds(i * step, step)
            kept = w_rows[n, pl.ds(core * half + i * step, step)].astype(F32)
            got = w_got[n, at].astype(F32)
            top, bottom = jnp.where(core == 0, kept, got), jnp.where(core == 0, got, kept)
            here[at] = jnp.concatenate([top, bottom], axis=1).astype(BF16)

        start(n)

    for n in range(6):
        across(n, at(n, 0, 0, 0))

    def row(k):
        for n in range(6):
            here = at(n, 0, 0, k)
            arrived(here, recv_c.at[n, k - 1])

            @pl.when(k < N - 1)
            def _(n=n, here=here):
                along_c(n, here, k)

            along_b(n, here, 0, k)
            along_a(n, here, 0, 0)
            across(n, here)

    def plane(j, k):
        for n in range(6):
            here = at(n, 0, j, k)
            arrived(here, recv_b.at[n, j - 1, k])

            @pl.when(j < N - 1)
            def _(n=n, here=here):
                along_b(n, here, j, k)

            along_a(n, here, 0, j)
            across(n, here)

    @pl.loop(1, 2 * N - 1)
    def _(far):
        @pl.loop(0, N)
        def _(j):
            k = far - j

            @pl.when((j == 0) & (k < N))
            def _():
                row(k)

            @pl.when((j > 0) & (k >= 0) & (k < N))
            def _():
                plane(j, k)

    def beyond(i, last):
        @pl.loop(0, N)
        def _(j):
            for n in range(6):
                here = at(n, i, j, None)
                arrived(here, recv_a.at[n, i - 1, j])
                if not last:
                    along_a(n, here, i, j)
                across(n, here)

    @pl.loop(1, N - 1)
    def _(i):
        beyond(i, False)

    for n in range(6):
        arrived(blocks(n, N**3), par_send.at[n])
    for n in range(4):
        arrived(g_send.at[n], swap_send.at[n])
        arrived(w_got.at[n], back_send.at[n])
    arrived(norm.at[0], norm_send.at[0, 0])
    for axis in range(3):
        for d in range(1, N):
            arrived(norm.at[0], norm_send.at[1 + axis, d - 1])

    beyond(N - 1, True)

    for n in range(6):
        arrived(blocks(n, N - 1), send_c.at[n])
        arrived(blocks(n, (N - 1) * N), send_b.at[n])
        arrived(blocks(n, (N - 1) * N * N), send_a.at[n])
        arrived(blocks(n, N**3), send_p.at[n])
        arrived(colored(n).at[:, :, :, theirs], recv_p.at[n])


def device_step(g, w, m, v, tiles):
    half = tiles // 2
    hbm, vmem = pl.BlockSpec(memory_space=pltpu.HBM), pl.BlockSpec(memory_space=pltpu.VMEM)
    dma = pltpu.SemaphoreType.DMA
    return pl.pallas_call(
        step_kernel,
        out_shape=[
            pltpu.VMEM((4, tiles, 4, 128), BF16),
            pltpu.VMEM((2, half, 8, 128), BF16),
            pltpu.VMEM((8, 128), F32),
            pltpu.VMEM((3, 2, N, N, N, tiles, 8, 128), BF16),
        ],
        in_specs=[hbm] * 12,
        out_specs=[vmem] * 4,
        scratch_shapes=[
            pltpu.VMEM((N, 6, N, half, 8, 128), BF16),
            pltpu.VMEM((4, half, 4, 128), BF16),
            pltpu.VMEM((4, tiles, 8, 128), BF16),
            pltpu.VMEM((2, half, 8, 128), BF16),
            pltpu.VMEM((4, tiles, 4, 128), BF16),
            pltpu.VMEM((4, half, 4, 128), BF16),
            pltpu.VMEM((4, tiles, 4, 128), F32),
            pltpu.VMEM((2, half, 8, 128), F32),
            pltpu.VMEM((4, tiles, 4, 128), F32),
            pltpu.VMEM((2, half, 8, 128), F32),
            pltpu.VMEM((5, 8, 128), F32),
            pltpu.VMEM((4, N - 1, 8, 128), F32),
            dma((N, 6)),
            dma((6,)),
            dma((6, N, N)),
            dma((6,)),
            dma((6, N - 1, N)),
            dma((6,)),
            dma((6, N - 1, N)),
            dma((6,)),
            dma((6, N - 1)),
            dma((4, N - 1)),
            dma((4, N - 1)),
            dma((4,)),
            dma((4,)),
            dma((4,)),
            dma((4,)),
            dma((12,)),
            dma((6,)),
            dma((6, N - 1)),
            dma((6,)),
            dma((6, N - 1, N)),
            dma((6,)),
            dma((6, N - 1, N)),
            dma((6,)),
            dma((6,)),
        ],
        compiler_params=pltpu.CompilerParams(collective_id=0, has_side_effects=True, vmem_limit_bytes=STEP_LIMIT),
        name="device_step",
    )(*g, *w, *m, *v)


def finish_kernel(w, g_wide, g_tall, factor, m0, m1, m2, v0, v1, v2, o0, o1, o2, nm0, nm1, nm2, nv0, nv1, nv2, sem):
    copies = [
        pltpu.make_async_copy(w.at[which, layer, x], dst.at[layer, x], sem.at[which, layer, x])
        for which, dst in enumerate((o0, o1, o2))
        for layer in range(2)
        for x in range(N)
    ]
    for copy in copies:
        copy.start()
    for which, (m, v, nm, nv) in enumerate(((m0, v0, nm0, nv0), (m1, v1, nm1, nv1), (m2, v2, nm2, nv2))):
        g = g_tall if which == 2 else g_wide.at[pl.ds(2 * which, 2)]
        for layer in range(2):

            @pl.loop(0, m.shape[1] // 8)
            def _(i, g=g, m=m, v=v, nm=nm, nv=nv, layer=layer):
                at = pl.ds(i * 8, 8)
                grad = g[layer, at].astype(F32)
                grad = grad * jnp.broadcast_to(factor[0:1, 0:1][:, :, None], grad.shape)
                nm[layer, at] = 0.9 * m[layer, at] + 0.1 * grad
                nv[layer, at] = 0.95 * v[layer, at] + 0.05 * grad * grad
    for copy in copies:
        copy.wait()


def finish(whole, g_wide, g_tall, factor, m, v):
    hbm, vmem = (pl.BlockSpec(memory_space=space) for space in (pltpu.HBM, pltpu.VMEM))
    whole_one = jax.ShapeDtypeStruct(whole.shape[1:], whole.dtype)
    like = [jax.ShapeDtypeStruct(one.shape, one.dtype) for one in (*[whole_one] * 3, *m, *v)]
    return pl.pallas_call(
        finish_kernel,
        out_shape=like,
        in_specs=[vmem] * 10,
        out_specs=[hbm] * 3 + [vmem] * 6,
        scratch_shapes=[pltpu.SemaphoreType.DMA((3, 2, N))],
        compiler_params=pltpu.CompilerParams(vmem_limit_bytes=FINISH_LIMIT),
        cost_estimate=pl.CostEstimate(flops=10**8, bytes_accessed=100 * 2**20, transcendentals=0),
        name="finish",
    )(whole, g_wide, g_tall, factor, *m, *v)


def wide_tiles(t, *major):
    rows = t.shape[-2] // functools.reduce(lambda a, b: a * b, major, 1)
    lead = t.shape[:-2]
    t = t.reshape(*lead, *major, rows, t.shape[-1] // 128, 128)
    return jnp.swapaxes(t, -3, -2)


def tall_tiles(t, *major):
    rows = t.shape[-2] // functools.reduce(lambda a, b: a * b, major, 1)
    lead = t.shape[:-2]
    t = t.reshape(*lead, *major, rows // 8, 8, t.shape[-1] // 128, 128)
    t = jnp.swapaxes(t, -3, -2)
    return t.reshape(*lead, *major, -1, 8, 128)


def from_wide(t, shape):
    return jnp.swapaxes(t, -3, -2).reshape(shape)


def from_tall(t, shape):
    columns = shape[-1] // 128
    t = t.reshape(*t.shape[:-3], t.shape[-3] // columns, columns, 8, 128)
    return jnp.swapaxes(t, -3, -2).reshape(shape)


def solution(mesh):
    def step(*arrays):
        terms, weights, m, v = (arrays[i : i + 3] for i in (0, 3, 6, 9))
        g = [wide_tiles(terms[0][0], N, N, N), wide_tiles(terms[1][0], N, N, N), tall_tiles(terms[2][0], N, N, N)]
        w = [wide_tiles(weights[0], N, N, N), wide_tiles(weights[1], N, N, N), tall_tiles(weights[2], N, N, N)]
        tiles = g[0].shape[4]

        def moments(one):
            return wide_tiles(one[0]), wide_tiles(one[1]), tall_tiles(one[2])

        m, v = moments(m), moments(v)
        g_wide, g_tall, factor, whole = device_step(g, w, m, v, tiles)
        new = finish(whole, g_wide, g_tall, factor, m, v)
        shapes = [one.shape for one in arrays[3:]]
        return tuple((from_tall if i % 3 == 2 else from_wide)(one, shape) for i, (one, shape) in enumerate(zip(new, shapes, strict=True)))

    all_of, cut = P(None, None, None), P(None, "dp", None)
    return jax.shard_map(
        step,
        mesh=mesh,
        in_specs=(P(("rep", "dp"), None, None, None),) * 3 + (all_of,) * 3 + (cut,) * 6,
        out_specs=(P("rep", None, None),) * 3 + (P("rep", "dp", None),) * 6,
        check_vma=False,
    )
```

```python
import functools

import jax
import jax.numpy as jnp
from jax import lax
from jax.experimental import pallas as pl
from jax.experimental.pallas import tpu as pltpu
from jax.sharding import PartitionSpec as P

N = 4
AHEAD = 2
STEP = 8
STEP_LIMIT, FINISH_LIMIT = 10 * 2**20, 4 * 2**20
DEVICES = 2 * N**3
ORDERS = ((0, 1, 2), (1, 2, 0), (2, 0, 1))
COLORS = tuple((which, layer) for which in range(3) for layer in range(2))
F32, BF16 = jnp.float32, jnp.bfloat16


def place():
    me = lax.axis_index("dp")
    chip = me // 2
    return lax.rem(me, 2), (chip // (N * N), lax.rem(chip // N, N), lax.rem(chip, N))


def device(core, chip):
    return {"dp": ((chip[0] * N + chip[1]) * N + chip[2]) * 2 + core}


def moved(chip, axis, by):
    return tuple(lax.rem(c + by + N, N) if a == axis else c for a, c in enumerate(chip))


def along(color, chip):
    which, layer = color
    axes = ORDERS[which]
    return axes, 1 - 2 * layer, tuple(chip[a] for a in axes)


def back(c, s, by):
    return lax.rem(c - s * by + N, N)


def block(ref, color, abc, tiles):
    axes = ORDERS[color[0]]
    where = [slice(None)] * 3
    for a, c in zip(axes, abc, strict=True):
        if c is not None:
            where[a] = c
    return ref.at[(color[1], *where, tiles)]


def send(src, dst, send_sem, recv_sem, to):
    copy = pltpu.make_async_remote_copy(
        src_ref=src, dst_ref=dst, send_sem=send_sem, recv_sem=recv_sem, device_id=to, device_id_type=pl.DeviceIdType.MESH
    )
    copy.start()
    return copy


def arrived(ref, sem):
    pltpu.make_async_copy(ref, ref, sem).wait()


def meet(peers):
    barrier = pltpu.get_barrier_semaphore()
    for peer in peers:
        pl.semaphore_signal(barrier, inc=1, device_id=peer, device_id_type=pl.DeviceIdType.MESH)
    pl.semaphore_wait(barrier, len(peers))


def add_up(out, ins, step):
    @pl.loop(0, out.shape[0] // step)
    def _(n):
        at = pl.ds(n * step, step)
        total = ins[0][at].astype(F32)
        for one in ins[1:]:
            total = total + one[at].astype(F32)
        out[at] = total.astype(out.dtype)


def step_kernel(
    g0, g1, g2, w0, w1, w2, m0, m1, m2, v0, v1, v2,
    m_wide, m_tall, v_wide, v_tall, whole,
    own, g_send, g_wide, g_tall, w_chip, w_chip_tall, w_rows, w_got, norm, norm_got,
    own_sem, par_send, par_recv, send1, recv1, send2, recv2, send3, recv3,
    norm_send, norm_recv, swap_send, swap_recv, back_send, back_recv, load_sem, send_p, recv_p,
):
    g, w = (g0, g1, g2), (w0, w1, w2)
    core, chip = place()
    half = own.shape[3]
    step = min(STEP, half)
    mine, theirs = pl.ds(core * half, half), pl.ds((1 - core) * half, half)
    low, high = pl.ds(0, half), pl.ds(half, half)
    partner = device(1 - core, chip)

    def colored(n):
        return whole.at[COLORS[n][0], COLORS[n][1]]

    def par(n, t, k):
        return colored(n).at[t, k, :, low]

    def r1(n, t, k):
        return colored(n).at[t, k, :, high]

    def r2(n, k):
        return colored(n).at[N - 1, k, :, high]

    def r3(n, j):
        return colored(n).at[N - 1, N - 1, j, high]

    def blocks(n, count):
        if count < N:
            return colored(n).at[0, 0, pl.ds(0, count), low]
        if count < N * N:
            return colored(n).at[0, pl.ds(0, count // N), :, low]
        return colored(n).at[pl.ds(0, count // (N * N)), :, :, low]

    def to(n, phase):
        axes, s, _ = along(COLORS[n], chip)
        return device(core, moved(chip, axes[phase], s))

    def targets(color, t, k):
        axes, s, (a, b, c) = along(color, chip)
        return back(a, s, t + 1), back(b, s, k + 1), None

    def own_copy(n, t, k):
        return pltpu.make_async_copy(block(g[COLORS[n][0]], COLORS[n], targets(COLORS[n], t, k), mine), own.at[k, n], own_sem.at[lax.rem(k, AHEAD), n])

    def push(n, t, k):
        src = block(g[COLORS[n][0]], COLORS[n], targets(COLORS[n], t, k), theirs)
        send(src, par(n, t, k), par_send.at[n], par_recv.at[n, k], partner)

    @pl.loop(0, AHEAD)
    def _(k):
        for n in range(6):
            own_copy(n, 0, k).start()

    meet([partner] + [device(core, moved(chip, axis, by)) for axis in range(3) for by in range(1, N)])

    @pl.loop(0, AHEAD)
    def _(k):
        for n in range(6):
            push(n, 0, k)

    loads = []
    for n, (which, layer) in enumerate(COLORS):
        if which < 2:
            loads.append((block(w[which], COLORS[n], along(COLORS[n], chip)[2], slice(None)), w_chip.at[n], 0))
        else:
            loads.append((block(w[which], COLORS[n], along(COLORS[n], chip)[2], mine), w_chip_tall.at[layer], 1))
    loads += [(m0, m_wide.at[pl.ds(0, 2)], 2), (m1, m_wide.at[pl.ds(2, 2)], 2), (m2, m_tall, 3)]
    loads += [(v0, v_wide.at[pl.ds(0, 2)], 4), (v1, v_wide.at[pl.ds(2, 2)], 4), (v2, v_tall, 5)]
    for src, dst, i in loads:
        pltpu.make_async_copy(src, dst, load_sem.at[i]).start()

    def ask(n, i):
        own_copy(n, i // N, lax.rem(i, N)).start()
        push(n, i // N, lax.rem(i, N))

    def ready(n, t, k):
        own_copy(n, t, k).wait()
        arrived(par(n, t, k), par_recv.at[n, k])

    def first_axis(n, t, k, first):
        ready(n, t, k)
        ins = [own.at[k, n], par(n, t, k)]
        if not first:
            arrived(r1(n, t - 1, k), recv1.at[n, t - 1, k])
            ins.append(r1(n, t - 1, k))

        @pl.loop(0, N)
        def _(q):
            add_up(par(n, t, k).at[q], [one.at[q] for one in ins], step)

        send(par(n, t, k), r1(n, t, k), send1.at[n], recv1.at[n, t, k], to(n, 0))
        ask(n, t * N + k + AHEAD)

    @pl.loop(0, N)
    def _(k):
        for n in range(6):
            first_axis(n, 0, k, True)

    @pl.loop(0, 2 * N)
    def _(i):
        for n in range(6):
            first_axis(n, 1 + i // N, lax.rem(i, N), False)

    def place_of(n, j):
        _, s, (_, _, c) = along(COLORS[n], chip)
        return back(c, s, j + 1 + (1 - j // 2) * (1 - 2 * j))

    def second_axis(n, k, j, first):
        at = place_of(n, j)
        ins = [own.at[k, n, at], par(n, N - 1, k).at[at], r1(n, N - 2, k).at[at]]
        if not first:
            arrived(r2(n, k - 1).at[at], recv2.at[n, k - 1, j])
            ins.append(r2(n, k - 1).at[at])
        out = par(n, N - 1, k).at[at]
        add_up(out, ins, step)
        send(out, r2(n, k).at[at], send2.at[n], recv2.at[n, k, j], to(n, 1))

    def second_axis_all(k, first):
        for n in range(6):
            ready(n, N - 1, k)
            arrived(r1(n, N - 2, k), recv1.at[n, N - 2, k])

            @pl.when(k + AHEAD < N)
            def _(n=n):
                ask(n, (N - 1) * N + k + AHEAD)

        @pl.loop(0, N)
        def _(j):
            for n in range(6):
                second_axis(n, k, j, first)

    second_axis_all(0, True)

    @pl.loop(1, N - 1)
    def _(k):
        second_axis_all(k, False)

    def third_axis_parts(n, j):
        k = N - 1
        at = place_of(n, j)
        arrived(r2(n, k - 1).at[at], recv2.at[n, k - 1, j])
        return [par(n, N - 1, k).at[at], own.at[k, n, at], r1(n, N - 2, k).at[at], r2(n, k - 1).at[at]]

    quarter = half // 2
    first_half, second_half = pl.ds(0, quarter), pl.ds(quarter, quarter)

    def to_third(n, s):
        return device(core, moved(chip, along(COLORS[n], chip)[0][2], s))

    def third_axis(n, parts, tiles, slot, sem, way, more=None):
        out = parts[0].at[tiles]
        add_up(out, [one.at[tiles] for one in parts] + ([] if more is None else [more]), step)
        send(out, r3(n, slot).at[tiles], send3.at[n], recv3.at[n, sem], to_third(n, way))

    up, down = [], []
    for n in range(6):
        s = 1 - 2 * COLORS[n][1]
        ready(n, N - 1, N - 1)
        arrived(r1(n, N - 2, N - 1), recv1.at[n, N - 2, N - 1])
        parts = third_axis_parts(n, 0)
        third_axis(n, parts, first_half, 0, 0, s)
        third_axis(n, parts, second_half, 0, 1, -s)
    for n in range(6):
        s = 1 - 2 * COLORS[n][1]
        up.append(third_axis_parts(n, 1))
        third_axis(n, up[n], first_half, 2, 3, -s)
        down.append(third_axis_parts(n, 2))
        third_axis(n, down[n], second_half, 1, 2, s)
    for n in range(6):
        s = 1 - 2 * COLORS[n][1]
        arrived(r3(n, 0).at[first_half], recv3.at[n, 0])
        third_axis(n, down[n], first_half, 1, 2, s, r3(n, 0).at[first_half])
        arrived(r3(n, 0).at[second_half], recv3.at[n, 1])
        third_axis(n, up[n], second_half, 2, 3, -s, r3(n, 0).at[second_half])

    norm[0] = jnp.zeros(norm.shape[1:], F32)
    for n, (which, layer) in enumerate(COLORS):
        ins = third_axis_parts(n, 3)
        for slot in (1, 2):
            arrived(r3(n, slot), recv3.at[n, slot + 1])
            ins.append(r3(n, slot))

        @pl.loop(0, half // step, init_carry=jnp.zeros(norm.shape[1:], F32))
        def squares(i, so_far, ins=ins, which=which, layer=layer, n=n):
            at = pl.ds(i * step, step)
            total = ins[0][at].astype(F32)
            for one in ins[1:]:
                total = total + one[at].astype(F32)
            rounded = total.astype(BF16)
            total = rounded.astype(F32)
            if which < 2:
                top, bottom = total[:, :4], total[:, 4:]
                g_wide[n, pl.ds(core * half + i * step, step)] = jnp.where(core == 0, top, bottom).astype(BF16)
                g_send[n, at] = jnp.where(core == 0, bottom, top).astype(BF16)
            else:
                g_tall[layer, at] = rounded
            return so_far + jnp.sum(total * total, axis=0)

        norm[0] += squares
        if which < 2:
            send(g_send.at[n], g_wide.at[n, mine], swap_send, swap_recv, partner)

    for n in range(6):
        arrived(blocks(n, (N - 1) * N * N), send1.at[n])
        arrived(blocks(n, (N - 1) * N), send2.at[n])
        arrived(blocks(n, N - 1), send3.at[n])

    send(norm.at[0], norm_got.at[0, 0], norm_send.at[0], norm_recv.at[0], partner)
    arrived(norm_got.at[0, 0], norm_recv.at[0])
    norm[1] = norm[0] + norm_got[0, 0]
    for axis in range(3):
        for d in range(1, N):
            src, dst = norm.at[1 + axis], norm_got.at[1 + axis, d - 1]
            send(src, dst, norm_send.at[1], norm_recv.at[1 + axis], device(core, moved(chip, axis, d)))
        if axis == 0:
            for i, dst in enumerate((w_chip, w_chip_tall, m_wide, m_tall, v_wide, v_tall)):
                arrived(dst, load_sem.at[i])
            arrived(g_wide.at[:, theirs], swap_recv)
        arrived(norm_got.at[1 + axis], norm_recv.at[1 + axis])
        total = norm[1 + axis]
        for d in range(1, N):
            total = total + norm_got[1 + axis, d - 1]
        norm[2 + axis] = total
    count = 6 * N**3 * 2 * half * 8 * 128
    everything = jnp.sum(norm[4], keepdims=True)
    factor = jnp.minimum(1.0, 0.5 * lax.rsqrt(everything / count + 1e-30))

    def new_weight(old, m, v, grad):
        m = 0.9 * m + 0.1 * grad
        v = 0.95 * v + 0.05 * grad * grad
        return (old - 0.02 * (m * lax.rsqrt(v + 1e-8) + 0.1 * old)).astype(BF16), m, v

    def at(n, i, j, k, tiles=mine):
        _, s, (a, b, c) = along(COLORS[n], chip)
        return block(whole.at[COLORS[n][0]], COLORS[n], (back(a, s, i), back(b, s, j), None if k is None else back(c, s, k)), tiles)

    def along_a(n, here, i, j):
        send(here, here, send1.at[n], recv1.at[n, i, j], to(n, 0))

    def along_b(n, here, j, k):
        send(here, here, send2.at[n], recv2.at[n, j, k], to(n, 1))

    def along_c(n, here, k):
        send(here, here, send3.at[n], recv3.at[n, k], to(n, 2))

    def across(n, here):
        send(here, here, send_p.at[n], recv_p.at[n], partner)

    def start(n):
        here = at(n, 0, 0, 0)
        along_c(n, here, 0)
        along_b(n, here, 0, 0)
        along_a(n, here, 0, 0)

    for n in range(4):

        @pl.loop(0, 2 * half // step)
        def _(i, n=n):
            at = pl.ds(i * step, step)
            old = w_chip[n, at].astype(F32)
            old = jnp.where(core == 0, old[:, :4], old[:, 4:])
            scale = jnp.broadcast_to(factor[:, :, None], old.shape)
            w_rows[n, at], m_wide[n, at], v_wide[n, at] = new_weight(old, m_wide[n, at], v_wide[n, at], g_wide[n, at].astype(F32) * scale)

        send(w_rows.at[n, theirs], w_got.at[n], back_send, back_recv.at[n], partner)

    for n in (4, 5):
        here = at(n, 0, 0, 0)

        @pl.loop(0, half // step)
        def _(i, layer=n - 4, here=here):
            at = pl.ds(i * step, step)
            old = w_chip_tall[layer, at].astype(F32)
            scale = jnp.broadcast_to(factor[:, :, None], old.shape)
            here[at], m_tall[layer, at], v_tall[layer, at] = new_weight(old, m_tall[layer, at], v_tall[layer, at], g_tall[layer, at].astype(F32) * scale)

        start(n)

    for n in range(4):
        here = at(n, 0, 0, 0)
        arrived(w_got.at[n], back_recv.at[n])

        @pl.loop(0, half // step)
        def _(i, n=n, here=here):
            at = pl.ds(i * step, step)
            kept = w_rows[n, pl.ds(core * half + i * step, step)].astype(F32)
            got = w_got[n, at].astype(F32)
            top, bottom = jnp.where(core == 0, kept, got), jnp.where(core == 0, got, kept)
            here[at] = jnp.concatenate([top, bottom], axis=1).astype(BF16)

        start(n)

    for n in range(6):
        across(n, at(n, 0, 0, 0))

    def row(k):
        for n in range(6):
            here = at(n, 0, 0, k)
            arrived(here, recv3.at[n, k - 1])

            @pl.when(k < N - 1)
            def _(n=n, here=here):
                along_c(n, here, k)

            along_b(n, here, 0, k)
            along_a(n, here, 0, 0)
            across(n, here)

    def plane(j, k):
        for n in range(6):
            here = at(n, 0, j, k)
            arrived(here, recv2.at[n, j - 1, k])

            @pl.when(j < N - 1)
            def _(n=n, here=here):
                along_b(n, here, j, k)

            along_a(n, here, 0, j)
            across(n, here)

    @pl.loop(1, 2 * N - 1)
    def _(far):
        @pl.loop(0, N)
        def _(j):
            k = far - j

            @pl.when((j == 0) & (k < N))
            def _():
                row(k)

            @pl.when((j > 0) & (k >= 0) & (k < N))
            def _():
                plane(j, k)

    def beyond(i, last):
        @pl.loop(0, N)
        def _(j):
            for n in range(6):
                here = at(n, i, j, None)
                arrived(here, recv1.at[n, i - 1, j])
                if not last:
                    along_a(n, here, i, j)
                across(n, here)

    @pl.loop(1, N - 1)
    def _(i):
        beyond(i, False)

    for n in range(6):
        arrived(blocks(n, N**3), par_send.at[n])
    arrived(g_send, swap_send)
    arrived(w_got, back_send)
    arrived(norm.at[0], norm_send.at[0])
    arrived(norm_got.at[pl.ds(1, 3)], norm_send.at[1])

    beyond(N - 1, True)

    for n in range(6):
        arrived(blocks(n, N - 1), send3.at[n])
        arrived(blocks(n, (N - 1) * N), send2.at[n])
        arrived(blocks(n, (N - 1) * N * N), send1.at[n])
        arrived(blocks(n, N**3), send_p.at[n])
        arrived(colored(n).at[:, :, :, theirs], recv_p.at[n])


def device_step(g, w, m, v, tiles):
    half = tiles // 2
    hbm, vmem = pl.BlockSpec(memory_space=pltpu.HBM), pl.BlockSpec(memory_space=pltpu.VMEM)
    dma = pltpu.SemaphoreType.DMA
    return pl.pallas_call(
        step_kernel,
        out_shape=[
            pltpu.VMEM((4, tiles, 4, 128), F32),
            pltpu.VMEM((2, half, 8, 128), F32),
            pltpu.VMEM((4, tiles, 4, 128), F32),
            pltpu.VMEM((2, half, 8, 128), F32),
            pltpu.VMEM((3, 2, N, N, N, tiles, 8, 128), BF16),
        ],
        in_specs=[hbm] * 12,
        out_specs=[vmem] * 5,
        scratch_shapes=[
            pltpu.VMEM((N, 6, N, half, 8, 128), BF16),
            pltpu.VMEM((4, half, 4, 128), BF16),
            pltpu.VMEM((4, tiles, 4, 128), BF16),
            pltpu.VMEM((2, half, 8, 128), BF16),
            pltpu.VMEM((4, tiles, 8, 128), BF16),
            pltpu.VMEM((2, half, 8, 128), BF16),
            pltpu.VMEM((4, tiles, 4, 128), BF16),
            pltpu.VMEM((4, half, 4, 128), BF16),
            pltpu.VMEM((5, 8, 128), F32),
            pltpu.VMEM((4, N - 1, 8, 128), F32),
            dma((AHEAD, 6)),
            dma((6,)),
            dma((6, N)),
            dma((6,)),
            dma((6, N - 1, N)),
            dma((6,)),
            dma((6, N - 1, N)),
            dma((6,)),
            dma((6, 4)),
            dma((2,)),
            dma((4,)),
            dma,
            dma,
            dma,
            dma((4,)),
            dma((6,)),
            dma((6,)),
            dma((6,)),
        ],
        compiler_params=pltpu.CompilerParams(collective_id=0, has_side_effects=True, vmem_limit_bytes=STEP_LIMIT),
        name="device_step",
    )(*g, *w, *m, *v)


def finish_kernel(m_wide, m_tall, v_wide, v_tall, w, *refs):
    out, sem = refs[:-1], refs[-1]
    copies = [(w.at[which, layer, x], out[which].at[layer, x]) for which in range(3) for layer in range(2) for x in range(N)]
    for first, wide, tall in ((3, m_wide, m_tall), (6, v_wide, v_tall)):
        copies += [(wide.at[pl.ds(0, 2)], out[first]), (wide.at[pl.ds(2, 2)], out[first + 1]), (tall, out[first + 2])]
    copies = [pltpu.make_async_copy(src, dst, sem.at[i]) for i, (src, dst) in enumerate(copies)]
    for copy in copies:
        copy.start()
    for copy in copies:
        copy.wait()


def finish(moments, whole, like):
    hbm, vmem = (pl.BlockSpec(memory_space=space) for space in (pltpu.HBM, pltpu.VMEM))
    one = jax.ShapeDtypeStruct(whole.shape[1:], whole.dtype)
    return pl.pallas_call(
        finish_kernel,
        out_shape=[one] * 3 + [jax.ShapeDtypeStruct(x.shape, x.dtype) for x in like],
        in_specs=[vmem] * 5,
        out_specs=[hbm] * 9,
        scratch_shapes=[pltpu.SemaphoreType.DMA((6 * N + 6,))],
        compiler_params=pltpu.CompilerParams(vmem_limit_bytes=FINISH_LIMIT),
        cost_estimate=pl.CostEstimate(flops=10**8, bytes_accessed=100 * 2**20, transcendentals=0),
        name="finish",
    )(*moments, whole)


def wide_tiles(t, *major):
    rows = t.shape[-2] // functools.reduce(lambda a, b: a * b, major, 1)
    lead = t.shape[:-2]
    t = t.reshape(*lead, *major, rows, t.shape[-1] // 128, 128)
    return jnp.swapaxes(t, -3, -2)


def tall_tiles(t, *major):
    rows = t.shape[-2] // functools.reduce(lambda a, b: a * b, major, 1)
    lead = t.shape[:-2]
    t = t.reshape(*lead, *major, rows // 8, 8, t.shape[-1] // 128, 128)
    t = jnp.swapaxes(t, -3, -2)
    return t.reshape(*lead, *major, -1, 8, 128)


def from_wide(t, shape):
    return jnp.swapaxes(t, -3, -2).reshape(shape)


def from_tall(t, shape):
    columns = shape[-1] // 128
    t = t.reshape(*t.shape[:-3], t.shape[-3] // columns, columns, 8, 128)
    return jnp.swapaxes(t, -3, -2).reshape(shape)


def solution(mesh):
    def step(*arrays):
        terms, weights, m, v = (arrays[i : i + 3] for i in (0, 3, 6, 9))
        g = [wide_tiles(terms[0][0], N, N, N), wide_tiles(terms[1][0], N, N, N), tall_tiles(terms[2][0], N, N, N)]
        w = [wide_tiles(weights[0], N, N, N), wide_tiles(weights[1], N, N, N), tall_tiles(weights[2], N, N, N)]
        tiles = g[0].shape[4]

        def moments(one):
            return wide_tiles(one[0]), wide_tiles(one[1]), tall_tiles(one[2])

        m, v = moments(m), moments(v)
        *new_moments, whole = device_step(g, w, m, v, tiles)
        new = finish(new_moments, whole, (*m, *v))
        shapes = [one.shape for one in arrays[3:]]
        return tuple((from_tall if i % 3 == 2 else from_wide)(one, shape) for i, (one, shape) in enumerate(zip(new, shapes, strict=True)))

    all_of, cut = P(None, None, None), P(None, "dp", None)
    return jax.shard_map(
        step,
        mesh=mesh,
        in_specs=(P(("rep", "dp"), None, None, None),) * 3 + (all_of,) * 3 + (cut,) * 6,
        out_specs=(P("rep", None, None),) * 3 + (P("rep", "dp", None),) * 6,
        check_vma=False,
    )
```

```python
import functools

import jax
import jax.numpy as jnp
from jax import lax
from jax.experimental import pallas as pl
from jax.experimental.pallas import tpu as pltpu
from jax.sharding import PartitionSpec as P

N = 4
AHEAD = 2
STEP = 8
STEP_LIMIT, FINISH_LIMIT = 10 * 2**20, 4 * 2**20
DEVICES = 2 * N**3
ORDERS = ((0, 1, 2), (1, 2, 0), (2, 0, 1))
COLORS = tuple((which, layer) for which in range(3) for layer in range(2))
F32, BF16 = jnp.float32, jnp.bfloat16


def place():
    me = lax.axis_index("dp")
    chip = me // 2
    return lax.rem(me, 2), (chip // (N * N), lax.rem(chip // N, N), lax.rem(chip, N))


def device(core, chip):
    return {"dp": ((chip[0] * N + chip[1]) * N + chip[2]) * 2 + core}


def moved(chip, axis, by):
    return tuple(lax.rem(c + by + N, N) if a == axis else c for a, c in enumerate(chip))


def along(color, chip):
    which, layer = color
    axes = ORDERS[which]
    return axes, 1 - 2 * layer, tuple(chip[a] for a in axes)


def back(c, s, by):
    return lax.rem(c - s * by + N, N)


def block(ref, color, abc, tiles):
    axes = ORDERS[color[0]]
    where = [slice(None)] * 3
    for a, c in zip(axes, abc, strict=True):
        if c is not None:
            where[a] = c
    return ref.at[(color[1], *where, tiles)]


def send(src, dst, send_sem, recv_sem, to):
    copy = pltpu.make_async_remote_copy(
        src_ref=src, dst_ref=dst, send_sem=send_sem, recv_sem=recv_sem, device_id=to, device_id_type=pl.DeviceIdType.MESH
    )
    copy.start()
    return copy


def arrived(ref, sem):
    pltpu.make_async_copy(ref, ref, sem).wait()


def meet(peers):
    barrier = pltpu.get_barrier_semaphore()
    for peer in peers:
        pl.semaphore_signal(barrier, inc=1, device_id=peer, device_id_type=pl.DeviceIdType.MESH)
    pl.semaphore_wait(barrier, len(peers))


def add_up(out, ins, step):
    @pl.loop(0, out.shape[0] // step)
    def _(n):
        at = pl.ds(n * step, step)
        total = ins[0][at].astype(F32)
        for one in ins[1:]:
            total = total + one[at].astype(F32)
        out[at] = total.astype(out.dtype)


def step_kernel(
    g0, g1, g2, w0, w1, w2, m0, m1, m2, v0, v1, v2,
    m_wide, m_tall, v_wide, v_tall, whole,
    own, g_send, g_wide, g_tall, w_chip, w_chip_tall, w_rows, w_got, norm, norm_got,
    own_sem, par_send, par_recv, send1, recv1, send2, recv2, send3, recv3,
    norm_send, norm_recv, swap_send, swap_recv, back_send, back_recv, load_sem, send_p, recv_p,
):
    g, w = (g0, g1, g2), (w0, w1, w2)
    core, chip = place()
    half = own.shape[3]
    step = min(STEP, half)
    mine, theirs = pl.ds(core * half, half), pl.ds((1 - core) * half, half)
    low, high = pl.ds(0, half), pl.ds(half, half)
    partner = device(1 - core, chip)

    def colored(n):
        return whole.at[COLORS[n][0], COLORS[n][1]]

    def par(n, t, k):
        return colored(n).at[t, k, :, low]

    def r1(n, t, k):
        return colored(n).at[t, k, :, high]

    def r2(n, k):
        return colored(n).at[N - 1, k, :, high]

    def r3(n, j):
        return colored(n).at[N - 1, N - 1, j, high]

    def blocks(n, count):
        if count < N:
            return colored(n).at[0, 0, pl.ds(0, count), low]
        if count < N * N:
            return colored(n).at[0, pl.ds(0, count // N), :, low]
        return colored(n).at[pl.ds(0, count // (N * N)), :, :, low]

    def to(n, phase):
        axes, s, _ = along(COLORS[n], chip)
        return device(core, moved(chip, axes[phase], s))

    def targets(color, t, k):
        axes, s, (a, b, c) = along(color, chip)
        return back(a, s, t + 1), back(b, s, k + 1), None

    def own_copy(n, t, k):
        return pltpu.make_async_copy(block(g[COLORS[n][0]], COLORS[n], targets(COLORS[n], t, k), mine), own.at[k, n], own_sem.at[lax.rem(k, AHEAD), n])

    def push(n, t, k):
        src = block(g[COLORS[n][0]], COLORS[n], targets(COLORS[n], t, k), theirs)
        send(src, par(n, t, k), par_send.at[n], par_recv.at[n, k], partner)

    @pl.loop(0, AHEAD)
    def _(k):
        for n in range(6):
            own_copy(n, 0, k).start()

    meet([partner] + [device(core, moved(chip, axis, by)) for axis in range(3) for by in (1, N - 1)])

    @pl.loop(0, AHEAD)
    def _(k):
        for n in range(6):
            push(n, 0, k)

    loads = []
    for n, (which, layer) in enumerate(COLORS):
        if which < 2:
            loads.append((block(w[which], COLORS[n], along(COLORS[n], chip)[2], slice(None)), w_chip.at[n], 0))
        else:
            loads.append((block(w[which], COLORS[n], along(COLORS[n], chip)[2], mine), w_chip_tall.at[layer], 1))
    loads += [(m0, m_wide.at[pl.ds(0, 2)], 2), (m1, m_wide.at[pl.ds(2, 2)], 2), (m2, m_tall, 3)]
    loads += [(v0, v_wide.at[pl.ds(0, 2)], 4), (v1, v_wide.at[pl.ds(2, 2)], 4), (v2, v_tall, 5)]
    for src, dst, i in loads:
        pltpu.make_async_copy(src, dst, load_sem.at[i]).start()

    def ask(n, i):
        own_copy(n, i // N, lax.rem(i, N)).start()
        push(n, i // N, lax.rem(i, N))

    def ready(n, t, k):
        own_copy(n, t, k).wait()
        arrived(par(n, t, k), par_recv.at[n, k])

    def first_axis(n, t, k, first):
        ready(n, t, k)
        ins = [own.at[k, n], par(n, t, k)]
        if not first:
            arrived(r1(n, t - 1, k), recv1.at[n, t - 1, k])
            ins.append(r1(n, t - 1, k))

        @pl.loop(0, N)
        def _(q):
            add_up(par(n, t, k).at[q], [one.at[q] for one in ins], step)

        send(par(n, t, k), r1(n, t, k), send1.at[n], recv1.at[n, t, k], to(n, 0))
        ask(n, t * N + k + AHEAD)

    @pl.loop(0, N)
    def _(k):
        for n in range(6):
            first_axis(n, 0, k, True)

    @pl.loop(0, 2 * N)
    def _(i):
        for n in range(6):
            first_axis(n, 1 + i // N, lax.rem(i, N), False)

    def place_of(n, j):
        _, s, (_, _, c) = along(COLORS[n], chip)
        return back(c, s, j + 1 + (1 - j // 2) * (1 - 2 * j))

    def second_axis(n, k, j, first):
        at = place_of(n, j)
        ins = [own.at[k, n, at], par(n, N - 1, k).at[at], r1(n, N - 2, k).at[at]]
        if not first:
            arrived(r2(n, k - 1).at[at], recv2.at[n, k - 1, j])
            ins.append(r2(n, k - 1).at[at])
        out = par(n, N - 1, k).at[at]
        add_up(out, ins, step)
        send(out, r2(n, k).at[at], send2.at[n], recv2.at[n, k, j], to(n, 1))

    def second_axis_all(k, first):
        for n in range(6):
            ready(n, N - 1, k)
            arrived(r1(n, N - 2, k), recv1.at[n, N - 2, k])

            @pl.when(k + AHEAD < N)
            def _(n=n):
                ask(n, (N - 1) * N + k + AHEAD)

        @pl.loop(0, N)
        def _(j):
            for n in range(6):
                second_axis(n, k, j, first)

    second_axis_all(0, True)

    @pl.loop(1, N - 1)
    def _(k):
        second_axis_all(k, False)

    def third_axis_parts(n, j):
        k = N - 1
        at = place_of(n, j)
        arrived(r2(n, k - 1).at[at], recv2.at[n, k - 1, j])
        return [par(n, N - 1, k).at[at], own.at[k, n, at], r1(n, N - 2, k).at[at], r2(n, k - 1).at[at]]

    quarter = half // 2
    first_half, second_half = pl.ds(0, quarter), pl.ds(quarter, quarter)

    def to_third(n, s):
        return device(core, moved(chip, along(COLORS[n], chip)[0][2], s))

    def third_axis(n, parts, tiles, slot, sem, way, more=None):
        out = parts[0].at[tiles]
        add_up(out, [one.at[tiles] for one in parts] + ([] if more is None else [more]), step)
        send(out, r3(n, slot).at[tiles], send3.at[n], recv3.at[n, sem], to_third(n, way))

    up, down = [], []
    for n in range(6):
        s = 1 - 2 * COLORS[n][1]
        ready(n, N - 1, N - 1)
        arrived(r1(n, N - 2, N - 1), recv1.at[n, N - 2, N - 1])
        parts = third_axis_parts(n, 0)
        third_axis(n, parts, first_half, 0, 0, s)
        third_axis(n, parts, second_half, 0, 1, -s)
    for n in range(6):
        s = 1 - 2 * COLORS[n][1]
        up.append(third_axis_parts(n, 1))
        third_axis(n, up[n], first_half, 2, 3, -s)
        down.append(third_axis_parts(n, 2))
        third_axis(n, down[n], second_half, 1, 2, s)
    for n in range(6):
        arrived(blocks(n, (N - 1) * N * N), send1.at[n])
        arrived(blocks(n, (N - 1) * N), send2.at[n])
    for n in range(6):
        s = 1 - 2 * COLORS[n][1]
        arrived(r3(n, 0).at[first_half], recv3.at[n, 0])
        third_axis(n, down[n], first_half, 1, 2, s, r3(n, 0).at[first_half])
        arrived(r3(n, 0).at[second_half], recv3.at[n, 1])
        third_axis(n, up[n], second_half, 2, 3, -s, r3(n, 0).at[second_half])

    norm[...] = jnp.zeros(norm.shape, F32)
    for n, (which, layer) in enumerate(COLORS):
        ins = third_axis_parts(n, 3)
        for slot in (1, 2):
            arrived(r3(n, slot), recv3.at[n, slot + 1])
            ins.append(r3(n, slot))

        @pl.loop(0, half // step, init_carry=jnp.zeros(norm.shape, F32))
        def squares(i, so_far, ins=ins, which=which, layer=layer, n=n):
            at = pl.ds(i * step, step)
            total = ins[0][at].astype(F32)
            for one in ins[1:]:
                total = total + one[at].astype(F32)
            rounded = total.astype(BF16)
            total = rounded.astype(F32)
            if which < 2:
                top, bottom = total[:, :4], total[:, 4:]
                g_wide[n, pl.ds(core * half + i * step, step)] = jnp.where(core == 0, top, bottom).astype(BF16)
                g_send[n, at] = jnp.where(core == 0, bottom, top).astype(BF16)
            else:
                g_tall[layer, at] = rounded
            return so_far + jnp.sum(total * total, axis=0)

        norm[...] += squares
        if which < 2:
            send(g_send.at[n], g_wide.at[n, mine], swap_send, swap_recv, partner)

    for n in range(6):
        arrived(blocks(n, N - 1), send3.at[n])

    me = lax.axis_index("dp")
    norm_got[me] = jnp.sum(norm[...], axis=0, keepdims=True)
    apart = DEVICES // N
    for first in (2 * apart, 3 * apart, apart, 0):

        @pl.loop(max(first, 1), first + apart)
        def _(d):
            send(norm_got.at[me], norm_got.at[me], norm_send, norm_recv, {"dp": lax.rem(me + d, DEVICES)})

    for i, dst in enumerate((w_chip, w_chip_tall, m_wide, m_tall, v_wide, v_tall)):
        arrived(dst, load_sem.at[i])
    arrived(g_wide.at[:, theirs], swap_recv)
    arrived(norm_got.at[pl.ds(0, DEVICES - 1)], norm_recv)
    count = 6 * N**3 * 2 * half * 8 * 128
    everything = jnp.sum(jnp.sum(norm_got[...], axis=0), keepdims=True)
    factor = jnp.minimum(1.0, 0.5 * lax.rsqrt(everything / count + 1e-30))

    def new_weight(old, m, v, grad):
        m = 0.9 * m + 0.1 * grad
        v = 0.95 * v + 0.05 * grad * grad
        return (old - 0.02 * (m * lax.rsqrt(v + 1e-8) + 0.1 * old)).astype(BF16), m, v

    def at(n, i, j, k, tiles=mine):
        _, s, (a, b, c) = along(COLORS[n], chip)
        return block(whole.at[COLORS[n][0]], COLORS[n], (back(a, s, i), back(b, s, j), None if k is None else back(c, s, k)), tiles)

    def along_a(n, here, i, j):
        send(here, here, send1.at[n], recv1.at[n, i, j], to(n, 0))

    def along_b(n, here, j, k):
        send(here, here, send2.at[n], recv2.at[n, j, k], to(n, 1))

    def along_c(n, here, k):
        send(here, here, send3.at[n], recv3.at[n, k], to(n, 2))

    def across(n, here):
        send(here, here, send_p.at[n], recv_p.at[n], partner)

    def start(n):
        here = at(n, 0, 0, 0)
        along_c(n, here, 0)
        along_b(n, here, 0, 0)
        along_a(n, here, 0, 0)

    def new_rows(n, first):
        at = pl.ds(first, step)
        old = w_chip[n, at].astype(F32)
        old = jnp.where(core == 0, old[:, :4], old[:, 4:])
        scale = jnp.broadcast_to(factor[:, :, None], old.shape)
        new, m_wide[n, at], v_wide[n, at] = new_weight(old, m_wide[n, at], v_wide[n, at], g_wide[n, at].astype(F32) * scale)
        return new

    for n in range(4):

        @pl.loop(0, half // step)
        def _(i, n=n):
            w_rows[n, pl.ds(i * step, step)] = new_rows(n, (1 - core) * half + i * step)

        send(w_rows.at[n], w_got.at[n], back_send, back_recv.at[n], partner)

    for n in (4, 5):
        here = at(n, 0, 0, 0)

        @pl.loop(0, half // step)
        def _(i, layer=n - 4, here=here):
            at = pl.ds(i * step, step)
            old = w_chip_tall[layer, at].astype(F32)
            scale = jnp.broadcast_to(factor[:, :, None], old.shape)
            here[at], m_tall[layer, at], v_tall[layer, at] = new_weight(old, m_tall[layer, at], v_tall[layer, at], g_tall[layer, at].astype(F32) * scale)

        start(n)

    for n in range(4):
        here = at(n, 0, 0, 0)
        arrived(w_got.at[n], back_recv.at[n])

        @pl.loop(0, half // step)
        def _(i, n=n, here=here):
            at = pl.ds(i * step, step)
            kept = new_rows(n, core * half + i * step).astype(F32)
            got = w_got[n, at].astype(F32)
            top, bottom = jnp.where(core == 0, kept, got), jnp.where(core == 0, got, kept)
            here[at] = jnp.concatenate([top, bottom], axis=1).astype(BF16)

        start(n)

    for n in range(6):
        across(n, at(n, 0, 0, 0))

    def row(k):
        for n in range(6):
            here = at(n, 0, 0, k)
            arrived(here, recv3.at[n, k - 1])

            @pl.when(k < N - 1)
            def _(n=n, here=here):
                along_c(n, here, k)

            along_b(n, here, 0, k)
            along_a(n, here, 0, 0)
            across(n, here)

    def plane(j, k):
        for n in range(6):
            here = at(n, 0, j, k)
            arrived(here, recv2.at[n, j - 1, k])

            @pl.when(j < N - 1)
            def _(n=n, here=here):
                along_b(n, here, j, k)

            along_a(n, here, 0, j)
            across(n, here)

    @pl.loop(1, 2 * N - 1)
    def _(far):
        @pl.loop(0, N)
        def _(j):
            k = far - j

            @pl.when((j == 0) & (k < N))
            def _():
                row(k)

            @pl.when((j > 0) & (k >= 0) & (k < N))
            def _():
                plane(j, k)

    def beyond(i, last):
        @pl.loop(0, N)
        def _(j):
            for n in range(6):
                here = at(n, i, j, None)
                arrived(here, recv1.at[n, i - 1, j])
                if not last:
                    along_a(n, here, i, j)
                across(n, here)

    @pl.loop(1, N - 1)
    def _(i):
        beyond(i, False)

    for n in range(6):
        arrived(blocks(n, N**3), par_send.at[n])
    arrived(g_send, swap_send)
    arrived(w_got, back_send)
    arrived(norm_got.at[pl.ds(0, DEVICES - 1)], norm_send)

    beyond(N - 1, True)

    for n in range(6):
        arrived(blocks(n, N - 1), send3.at[n])
        arrived(blocks(n, (N - 1) * N), send2.at[n])
        arrived(blocks(n, (N - 1) * N * N), send1.at[n])
        arrived(blocks(n, N**3), send_p.at[n])
        arrived(colored(n).at[:, :, :, theirs], recv_p.at[n])


def device_step(g, w, m, v, tiles):
    half = tiles // 2
    hbm, vmem = pl.BlockSpec(memory_space=pltpu.HBM), pl.BlockSpec(memory_space=pltpu.VMEM)
    dma = pltpu.SemaphoreType.DMA
    return pl.pallas_call(
        step_kernel,
        out_shape=[
            pltpu.VMEM((4, tiles, 4, 128), F32),
            pltpu.VMEM((2, half, 8, 128), F32),
            pltpu.VMEM((4, tiles, 4, 128), F32),
            pltpu.VMEM((2, half, 8, 128), F32),
            pltpu.VMEM((3, 2, N, N, N, tiles, 8, 128), BF16),
        ],
        in_specs=[hbm] * 12,
        out_specs=[vmem] * 5,
        scratch_shapes=[
            pltpu.VMEM((N, 6, N, half, 8, 128), BF16),
            pltpu.VMEM((4, half, 4, 128), BF16),
            pltpu.VMEM((4, tiles, 4, 128), BF16),
            pltpu.VMEM((2, half, 8, 128), BF16),
            pltpu.VMEM((4, tiles, 8, 128), BF16),
            pltpu.VMEM((2, half, 8, 128), BF16),
            pltpu.VMEM((4, half, 4, 128), BF16),
            pltpu.VMEM((4, half, 4, 128), BF16),
            pltpu.VMEM((8, 128), F32),
            pltpu.VMEM((DEVICES, 1, 128), F32),
            dma((AHEAD, 6)),
            dma((6,)),
            dma((6, N)),
            dma((6,)),
            dma((6, N - 1, N)),
            dma((6,)),
            dma((6, N - 1, N)),
            dma((6,)),
            dma((6, 4)),
            dma,
            dma,
            dma,
            dma,
            dma,
            dma((4,)),
            dma((6,)),
            dma((6,)),
            dma((6,)),
        ],
        compiler_params=pltpu.CompilerParams(collective_id=0, has_side_effects=True, vmem_limit_bytes=STEP_LIMIT),
        name="device_step",
    )(*g, *w, *m, *v)


def finish_kernel(m_wide, m_tall, v_wide, v_tall, w, *refs):
    out, sem = refs[:-1], refs[-1]
    copies = [(w.at[which, layer, x], out[which].at[layer, x]) for which in range(3) for layer in range(2) for x in range(N)]
    for first, wide, tall in ((3, m_wide, m_tall), (6, v_wide, v_tall)):
        copies += [(wide.at[pl.ds(0, 2)], out[first]), (wide.at[pl.ds(2, 2)], out[first + 1]), (tall, out[first + 2])]
    copies = [pltpu.make_async_copy(src, dst, sem.at[i]) for i, (src, dst) in enumerate(copies)]
    for copy in copies:
        copy.start()
    for copy in copies:
        copy.wait()


def finish(moments, whole, like):
    hbm, vmem = (pl.BlockSpec(memory_space=space) for space in (pltpu.HBM, pltpu.VMEM))
    one = jax.ShapeDtypeStruct(whole.shape[1:], whole.dtype)
    return pl.pallas_call(
        finish_kernel,
        out_shape=[one] * 3 + [jax.ShapeDtypeStruct(x.shape, x.dtype) for x in like],
        in_specs=[vmem] * 5,
        out_specs=[hbm] * 9,
        scratch_shapes=[pltpu.SemaphoreType.DMA((6 * N + 6,))],
        compiler_params=pltpu.CompilerParams(vmem_limit_bytes=FINISH_LIMIT),
        cost_estimate=pl.CostEstimate(flops=10**8, bytes_accessed=100 * 2**20, transcendentals=0),
        name="finish",
    )(*moments, whole)


def wide_tiles(t, *major):
    rows = t.shape[-2] // functools.reduce(lambda a, b: a * b, major, 1)
    lead = t.shape[:-2]
    t = t.reshape(*lead, *major, rows, t.shape[-1] // 128, 128)
    return jnp.swapaxes(t, -3, -2)


def tall_tiles(t, *major):
    rows = t.shape[-2] // functools.reduce(lambda a, b: a * b, major, 1)
    lead = t.shape[:-2]
    t = t.reshape(*lead, *major, rows // 8, 8, t.shape[-1] // 128, 128)
    t = jnp.swapaxes(t, -3, -2)
    return t.reshape(*lead, *major, -1, 8, 128)


def from_wide(t, shape):
    return jnp.swapaxes(t, -3, -2).reshape(shape)


def from_tall(t, shape):
    columns = shape[-1] // 128
    t = t.reshape(*t.shape[:-3], t.shape[-3] // columns, columns, 8, 128)
    return jnp.swapaxes(t, -3, -2).reshape(shape)


def solution(mesh):
    def step(*arrays):
        terms, weights, m, v = (arrays[i : i + 3] for i in (0, 3, 6, 9))
        g = [wide_tiles(terms[0][0], N, N, N), wide_tiles(terms[1][0], N, N, N), tall_tiles(terms[2][0], N, N, N)]
        w = [wide_tiles(weights[0], N, N, N), wide_tiles(weights[1], N, N, N), tall_tiles(weights[2], N, N, N)]
        tiles = g[0].shape[4]

        def moments(one):
            return wide_tiles(one[0]), wide_tiles(one[1]), tall_tiles(one[2])

        m, v = moments(m), moments(v)
        *new_moments, whole = device_step(g, w, m, v, tiles)
        new = finish(new_moments, whole, (*m, *v))
        shapes = [one.shape for one in arrays[3:]]
        return tuple((from_tall if i % 3 == 2 else from_wide)(one, shape) for i, (one, shape) in enumerate(zip(new, shapes, strict=True)))

    all_of, cut = P(None, None, None), P(None, "dp", None)
    return jax.shard_map(
        step,
        mesh=mesh,
        in_specs=(P(("rep", "dp"), None, None, None),) * 3 + (all_of,) * 3 + (cut,) * 6,
        out_specs=(P("rep", None, None),) * 3 + (P("rep", "dp", None),) * 6,
        check_vma=False,
    )
```

```python
import functools

import jax
import jax.numpy as jnp
from jax import lax
from jax.experimental import pallas as pl
from jax.experimental.pallas import tpu as pltpu
from jax.sharding import PartitionSpec as P

N = 4
AHEAD = 2
STEP = 32
STEP_LIMIT, FINISH_LIMIT = 10 * 2**20, 4 * 2**20
DEVICES = 2 * N**3
ORDERS = ((0, 1, 2), (1, 2, 0), (2, 0, 1))
COLORS = tuple((which, layer) for which in range(3) for layer in range(2))
F32, BF16 = jnp.float32, jnp.bfloat16


def place():
    me = lax.axis_index("dp")
    chip = me // 2
    return lax.rem(me, 2), (chip // (N * N), lax.rem(chip // N, N), lax.rem(chip, N))


def device(core, chip):
    return {"dp": ((chip[0] * N + chip[1]) * N + chip[2]) * 2 + core}


def moved(chip, axis, by):
    return tuple(lax.rem(c + by + N, N) if a == axis else c for a, c in enumerate(chip))


def along(color, chip):
    which, layer = color
    axes = ORDERS[which]
    return axes, 1 - 2 * layer, tuple(chip[a] for a in axes)


def back(c, s, by):
    return lax.rem(c - s * by + N, N)


def block(ref, color, abc, tiles):
    axes = ORDERS[color[0]]
    where = [slice(None)] * 3
    for a, c in zip(axes, abc, strict=True):
        if c is not None:
            where[a] = c
    return ref.at[(color[1], *where, tiles)]


def send(src, dst, send_sem, recv_sem, to):
    copy = pltpu.make_async_remote_copy(
        src_ref=src, dst_ref=dst, send_sem=send_sem, recv_sem=recv_sem, device_id=to, device_id_type=pl.DeviceIdType.MESH
    )
    copy.start()
    return copy


def arrived(ref, sem):
    pltpu.make_async_copy(ref, ref, sem).wait()


def meet(peers):
    barrier = pltpu.get_barrier_semaphore()
    for peer in peers:
        pl.semaphore_signal(barrier, inc=1, device_id=peer, device_id_type=pl.DeviceIdType.MESH)
    pl.semaphore_wait(barrier, len(peers))


def add_up(out, ins, step):
    step = min(step, out.shape[0])

    @pl.loop(0, out.shape[0] // step)
    def _(n):
        at = pl.ds(n * step, step)
        total = ins[0][at].astype(F32)
        for one in ins[1:]:
            total = total + one[at].astype(F32)
        out[at] = total.astype(out.dtype)


def step_kernel(
    g0, g1, g2, w0, w1, w2, m0, m1, m2, v0, v1, v2,
    m_wide, m_tall, v_wide, v_tall, whole,
    own, g_send, g_wide, g_tall, w_chip, w_chip_tall, w_rows, w_got, norm, norm_got,
    own_sem, par_send, par_recv, send1, recv1, send2, recv2, send3, recv3,
    norm_send, norm_recv, swap_send, swap_recv, back_send, back_recv, load_sem, send_p, recv_p, first_recv,
):
    g, w = (g0, g1, g2), (w0, w1, w2)
    core, chip = place()
    half = own.shape[3]
    step = min(STEP, half)
    mine, theirs = pl.ds(core * half, half), pl.ds((1 - core) * half, half)
    low, high = pl.ds(0, half), pl.ds(half, half)
    partner = device(1 - core, chip)

    def colored(n):
        return whole.at[COLORS[n][0], COLORS[n][1]]

    def par(n, t, k):
        return colored(n).at[t, k, :, low]

    def r1(n, t, k):
        return colored(n).at[t, k, :, high]

    def r2(n, k):
        return colored(n).at[N - 1, k, :, high]

    def r3(n, j):
        return colored(n).at[N - 1, N - 1, j, high]

    def blocks(n, count):
        if count < N:
            return colored(n).at[0, 0, pl.ds(0, count), low]
        if count < N * N:
            return colored(n).at[0, pl.ds(0, count // N), :, low]
        return colored(n).at[pl.ds(0, count // (N * N)), :, :, low]

    def to(n, phase):
        axes, s, _ = along(COLORS[n], chip)
        return device(core, moved(chip, axes[phase], s))

    def targets(color, t, k):
        axes, s, (a, b, c) = along(color, chip)
        return back(a, s, t + 1), back(b, s, k + 1), None

    def own_copy(n, t, k):
        return pltpu.make_async_copy(block(g[COLORS[n][0]], COLORS[n], targets(COLORS[n], t, k), mine), own.at[k, n], own_sem.at[lax.rem(k, AHEAD), n])

    def push(n, t, k):
        src = block(g[COLORS[n][0]], COLORS[n], targets(COLORS[n], t, k), theirs)
        send(src, par(n, t, k), par_send.at[n], par_recv.at[n, k], partner)

    @pl.loop(0, AHEAD)
    def _(k):
        for n in range(6):
            own_copy(n, 0, k).start()

    meet([partner] + [device(core, moved(chip, axis, by)) for axis in range(3) for by in (1, N - 1)])

    @pl.loop(0, N)
    def _(q):
        for n in range(6):
            a, b, _ = targets(COLORS[n], 0, 0)
            src = block(g[COLORS[n][0]], COLORS[n], (a, b, q), theirs)
            send(src, par(n, 0, 0).at[q], par_send.at[n], first_recv.at[n, q], partner)

    @pl.loop(1, AHEAD)
    def _(k):
        for n in range(6):
            push(n, 0, k)

    loads = []
    for n, (which, layer) in enumerate(COLORS):
        if which < 2:
            loads.append((block(w[which], COLORS[n], along(COLORS[n], chip)[2], slice(None)), w_chip.at[n], 0))
        else:
            loads.append((block(w[which], COLORS[n], along(COLORS[n], chip)[2], mine), w_chip_tall.at[layer], 1))
    loads += [(m0, m_wide.at[pl.ds(0, 2)], 2), (m1, m_wide.at[pl.ds(2, 2)], 2), (m2, m_tall, 3)]
    loads += [(v0, v_wide.at[pl.ds(0, 2)], 4), (v1, v_wide.at[pl.ds(2, 2)], 4), (v2, v_tall, 5)]
    for src, dst, i in loads:
        pltpu.make_async_copy(src, dst, load_sem.at[i]).start()

    def ask(n, i):
        own_copy(n, i // N, lax.rem(i, N)).start()
        push(n, i // N, lax.rem(i, N))

    def ready(n, t, k):
        own_copy(n, t, k).wait()
        arrived(par(n, t, k), par_recv.at[n, k])

    def first_axis(n, t, k, first):
        ready(n, t, k)
        ins = [own.at[k, n], par(n, t, k)]
        if not first:
            arrived(r1(n, t - 1, k), recv1.at[n, t - 1, k])
            ins.append(r1(n, t - 1, k))

        @pl.loop(0, N)
        def _(q):
            add_up(par(n, t, k).at[q], [one.at[q] for one in ins], step)

        send(par(n, t, k), r1(n, t, k), send1.at[n], recv1.at[n, t, k], to(n, 0))
        ask(n, t * N + k + AHEAD)

    for n in range(6):
        own_copy(n, 0, 0).wait()

    @pl.loop(0, N)
    def _(q):
        for n in range(6):
            out = par(n, 0, 0).at[q]
            arrived(out, first_recv.at[n, q])
            add_up(out, [own.at[0, n, q], out], step)
            send(out, r1(n, 0, 0).at[q], send1.at[n], recv1.at[n, 0, 0], to(n, 0))

    for n in range(6):
        ask(n, AHEAD)

    @pl.loop(1, N)
    def _(k):
        for n in range(6):
            first_axis(n, 0, k, True)

    @pl.loop(0, 2 * N)
    def _(i):
        for n in range(6):
            first_axis(n, 1 + i // N, lax.rem(i, N), False)

    def place_of(n, j):
        _, s, (_, _, c) = along(COLORS[n], chip)
        return back(c, s, j + 1 + (1 - j // 2) * (1 - 2 * j))

    def second_axis(n, k, j, first):
        at = place_of(n, j)
        ins = [own.at[k, n, at], par(n, N - 1, k).at[at], r1(n, N - 2, k).at[at]]
        if not first:
            arrived(r2(n, k - 1).at[at], recv2.at[n, k - 1, j])
            ins.append(r2(n, k - 1).at[at])
        out = par(n, N - 1, k).at[at]
        add_up(out, ins, step)
        send(out, r2(n, k).at[at], send2.at[n], recv2.at[n, k, j], to(n, 1))

    def second_axis_all(k, first):
        for n in range(6):
            ready(n, N - 1, k)
            arrived(r1(n, N - 2, k), recv1.at[n, N - 2, k])

            @pl.when(k + AHEAD < N)
            def _(n=n):
                ask(n, (N - 1) * N + k + AHEAD)

        @pl.loop(0, N)
        def _(j):
            for n in range(6):
                second_axis(n, k, j, first)

    second_axis_all(0, True)

    @pl.loop(1, N - 1)
    def _(k):
        second_axis_all(k, False)

    def third_axis_parts(n, j):
        k = N - 1
        at = place_of(n, j)
        arrived(r2(n, k - 1).at[at], recv2.at[n, k - 1, j])
        return [par(n, N - 1, k).at[at], own.at[k, n, at], r1(n, N - 2, k).at[at], r2(n, k - 1).at[at]]

    quarter = half // 2
    first_half, second_half = pl.ds(0, quarter), pl.ds(quarter, quarter)

    def to_third(n, s):
        return device(core, moved(chip, along(COLORS[n], chip)[0][2], s))

    def third_axis(n, parts, tiles, slot, sem, way, more=None):
        out = parts[0].at[tiles]
        add_up(out, [one.at[tiles] for one in parts] + ([] if more is None else [more]), step)
        send(out, r3(n, slot).at[tiles], send3.at[n], recv3.at[n, sem], to_third(n, way))

    up, down = [], []
    for n in range(6):
        s = 1 - 2 * COLORS[n][1]
        ready(n, N - 1, N - 1)
        arrived(r1(n, N - 2, N - 1), recv1.at[n, N - 2, N - 1])
        parts = third_axis_parts(n, 0)
        third_axis(n, parts, first_half, 0, 0, s)
        third_axis(n, parts, second_half, 0, 1, -s)
    for n in range(6):
        s = 1 - 2 * COLORS[n][1]
        up.append(third_axis_parts(n, 1))
        third_axis(n, up[n], first_half, 2, 3, -s)
        down.append(third_axis_parts(n, 2))
        third_axis(n, down[n], second_half, 1, 2, s)
    for n in range(6):
        arrived(blocks(n, (N - 1) * N * N), send1.at[n])
        arrived(blocks(n, (N - 1) * N), send2.at[n])
    for n in range(6):
        s = 1 - 2 * COLORS[n][1]
        arrived(r3(n, 0).at[first_half], recv3.at[n, 0])
        third_axis(n, down[n], first_half, 1, 2, s, r3(n, 0).at[first_half])
        arrived(r3(n, 0).at[second_half], recv3.at[n, 1])
        third_axis(n, up[n], second_half, 2, 3, -s, r3(n, 0).at[second_half])

    norm[...] = jnp.zeros(norm.shape, F32)
    for n, (which, layer) in enumerate(COLORS):
        ins = third_axis_parts(n, 3)
        for slot in (1, 2):
            arrived(r3(n, slot), recv3.at[n, slot + 1])
            ins.append(r3(n, slot))

        @pl.loop(0, half // step, init_carry=jnp.zeros(norm.shape, F32))
        def squares(i, so_far, ins=ins, which=which, layer=layer, n=n):
            at = pl.ds(i * step, step)
            total = ins[0][at].astype(F32)
            for one in ins[1:]:
                total = total + one[at].astype(F32)
            rounded = total.astype(BF16)
            total = rounded.astype(F32)
            if which < 2:
                top, bottom = total[:, :4], total[:, 4:]
                g_wide[n, pl.ds(core * half + i * step, step)] = jnp.where(core == 0, top, bottom).astype(BF16)
                g_send[n, at] = jnp.where(core == 0, bottom, top).astype(BF16)
            else:
                g_tall[layer, at] = rounded
            return so_far + jnp.sum(total * total, axis=0)

        norm[...] += squares
        if which < 2:
            send(g_send.at[n], g_wide.at[n, mine], swap_send, swap_recv, partner)

    for n in range(6):
        arrived(blocks(n, N - 1), send3.at[n])

    me = lax.axis_index("dp")
    norm_got[me] = jnp.sum(norm[...], axis=0, keepdims=True)
    apart = DEVICES // N
    for first in (2 * apart, 3 * apart, apart, 0):

        @pl.loop(max(first, 1), first + apart)
        def _(d):
            send(norm_got.at[me], norm_got.at[me], norm_send, norm_recv, {"dp": lax.rem(me + d, DEVICES)})

    for i, dst in enumerate((w_chip, w_chip_tall, m_wide, m_tall, v_wide, v_tall)):
        arrived(dst, load_sem.at[i])
    arrived(g_wide.at[:, theirs], swap_recv)
    arrived(norm_got.at[pl.ds(0, DEVICES - 1)], norm_recv)
    count = 6 * N**3 * 2 * half * 8 * 128
    everything = jnp.sum(jnp.sum(norm_got[...], axis=0), keepdims=True)
    factor = jnp.minimum(1.0, 0.5 * lax.rsqrt(everything / count + 1e-30))

    def new_weight(old, m, v, grad):
        m = 0.9 * m + 0.1 * grad
        v = 0.95 * v + 0.05 * grad * grad
        return (old - 0.02 * (m * lax.rsqrt(v + 1e-8) + 0.1 * old)).astype(BF16), m, v

    def at(n, i, j, k, tiles=mine):
        _, s, (a, b, c) = along(COLORS[n], chip)
        return block(whole.at[COLORS[n][0]], COLORS[n], (back(a, s, i), back(b, s, j), None if k is None else back(c, s, k)), tiles)

    def along_a(n, here, i, j):
        send(here, here, send1.at[n], recv1.at[n, i, j], to(n, 0))

    def along_b(n, here, j, k):
        send(here, here, send2.at[n], recv2.at[n, j, k], to(n, 1))

    def along_c(n, here, k):
        send(here, here, send3.at[n], recv3.at[n, k], to(n, 2))

    def across(n, here):
        send(here, here, send_p.at[n], recv_p.at[n], partner)

    def start(n):
        here = at(n, 0, 0, 0)
        along_c(n, here, 0)
        along_b(n, here, 0, 0)
        along_a(n, here, 0, 0)

    def new_rows(n, first):
        at = pl.ds(first, step)
        old = w_chip[n, at].astype(F32)
        old = jnp.where(core == 0, old[:, :4], old[:, 4:])
        scale = jnp.broadcast_to(factor[:, :, None], old.shape)
        new, m_wide[n, at], v_wide[n, at] = new_weight(old, m_wide[n, at], v_wide[n, at], g_wide[n, at].astype(F32) * scale)
        return new

    for n in range(4):

        @pl.loop(0, half // step)
        def _(i, n=n):
            w_rows[n, pl.ds(i * step, step)] = new_rows(n, (1 - core) * half + i * step)

        send(w_rows.at[n], w_got.at[n], back_send, back_recv.at[n], partner)

    for n in (4, 5):
        here = at(n, 0, 0, 0)

        @pl.loop(0, half // step)
        def _(i, layer=n - 4, here=here):
            at = pl.ds(i * step, step)
            old = w_chip_tall[layer, at].astype(F32)
            scale = jnp.broadcast_to(factor[:, :, None], old.shape)
            here[at], m_tall[layer, at], v_tall[layer, at] = new_weight(old, m_tall[layer, at], v_tall[layer, at], g_tall[layer, at].astype(F32) * scale)

        start(n)

    for n in range(4):
        here = at(n, 0, 0, 0)
        arrived(w_got.at[n], back_recv.at[n])

        @pl.loop(0, half // step)
        def _(i, n=n, here=here):
            at = pl.ds(i * step, step)
            kept = new_rows(n, core * half + i * step).astype(F32)
            got = w_got[n, at].astype(F32)
            top, bottom = jnp.where(core == 0, kept, got), jnp.where(core == 0, got, kept)
            here[at] = jnp.concatenate([top, bottom], axis=1).astype(BF16)

        start(n)

    for n in range(6):
        across(n, at(n, 0, 0, 0))

    def row(k):
        for n in range(6):
            here = at(n, 0, 0, k)
            arrived(here, recv3.at[n, k - 1])

            @pl.when(k < N - 1)
            def _(n=n, here=here):
                along_c(n, here, k)

            along_b(n, here, 0, k)
            along_a(n, here, 0, 0)
            across(n, here)

    def plane(j, k):
        for n in range(6):
            here = at(n, 0, j, k)
            arrived(here, recv2.at[n, j - 1, k])

            @pl.when(j < N - 1)
            def _(n=n, here=here):
                along_b(n, here, j, k)

            along_a(n, here, 0, j)
            across(n, here)

    @pl.loop(1, 2 * N - 1)
    def _(far):
        @pl.loop(0, N)
        def _(j):
            k = far - j

            @pl.when((j == 0) & (k < N))
            def _():
                row(k)

            @pl.when((j > 0) & (k >= 0) & (k < N))
            def _():
                plane(j, k)

    def beyond(i, last):
        @pl.loop(0, N)
        def _(j):
            for n in range(6):
                here = at(n, i, j, None)
                arrived(here, recv1.at[n, i - 1, j])
                if not last:
                    along_a(n, here, i, j)
                across(n, here)

    @pl.loop(1, N - 1)
    def _(i):
        beyond(i, False)

    for n in range(6):
        arrived(blocks(n, N**3), par_send.at[n])
    arrived(g_send, swap_send)
    arrived(w_got, back_send)
    arrived(norm_got.at[pl.ds(0, DEVICES - 1)], norm_send)

    beyond(N - 1, True)

    for n in range(6):
        arrived(blocks(n, N - 1), send3.at[n])
        arrived(blocks(n, (N - 1) * N), send2.at[n])
        arrived(blocks(n, (N - 1) * N * N), send1.at[n])
        arrived(blocks(n, N**3), send_p.at[n])
        arrived(colored(n).at[:, :, :, theirs], recv_p.at[n])


def device_step(g, w, m, v, tiles):
    half = tiles // 2
    hbm, vmem = pl.BlockSpec(memory_space=pltpu.HBM), pl.BlockSpec(memory_space=pltpu.VMEM)
    dma = pltpu.SemaphoreType.DMA
    return pl.pallas_call(
        step_kernel,
        out_shape=[
            pltpu.VMEM((4, tiles, 4, 128), F32),
            pltpu.VMEM((2, half, 8, 128), F32),
            pltpu.VMEM((4, tiles, 4, 128), F32),
            pltpu.VMEM((2, half, 8, 128), F32),
            pltpu.VMEM((3, 2, N, N, N, tiles, 8, 128), BF16),
        ],
        in_specs=[hbm] * 12,
        out_specs=[vmem] * 5,
        scratch_shapes=[
            pltpu.VMEM((N, 6, N, half, 8, 128), BF16),
            pltpu.VMEM((4, half, 4, 128), BF16),
            pltpu.VMEM((4, tiles, 4, 128), BF16),
            pltpu.VMEM((2, half, 8, 128), BF16),
            pltpu.VMEM((4, tiles, 8, 128), BF16),
            pltpu.VMEM((2, half, 8, 128), BF16),
            pltpu.VMEM((4, half, 4, 128), BF16),
            pltpu.VMEM((4, half, 4, 128), BF16),
            pltpu.VMEM((8, 128), F32),
            pltpu.VMEM((DEVICES, 1, 128), F32),
            dma((AHEAD, 6)),
            dma((6,)),
            dma((6, N)),
            dma((6,)),
            dma((6, N - 1, N)),
            dma((6,)),
            dma((6, N - 1, N)),
            dma((6,)),
            dma((6, 4)),
            dma,
            dma,
            dma,
            dma,
            dma,
            dma((4,)),
            dma((6,)),
            dma((6,)),
            dma((6,)),
            dma((6, N)),
        ],
        compiler_params=pltpu.CompilerParams(collective_id=0, has_side_effects=True, vmem_limit_bytes=STEP_LIMIT),
        name="device_step",
    )(*g, *w, *m, *v)


def finish_kernel(m_wide, m_tall, v_wide, v_tall, w, *refs):
    out, sem = refs[:-1], refs[-1]
    copies = [(w.at[which, layer, x], out[which].at[layer, x]) for which in range(3) for layer in range(2) for x in range(N)]
    for first, wide, tall in ((3, m_wide, m_tall), (6, v_wide, v_tall)):
        copies += [(wide.at[pl.ds(0, 2)], out[first]), (wide.at[pl.ds(2, 2)], out[first + 1]), (tall, out[first + 2])]
    copies = [pltpu.make_async_copy(src, dst, sem.at[i]) for i, (src, dst) in enumerate(copies)]
    for copy in copies:
        copy.start()
    for copy in copies:
        copy.wait()


def finish(moments, whole, like):
    hbm, vmem = (pl.BlockSpec(memory_space=space) for space in (pltpu.HBM, pltpu.VMEM))
    one = jax.ShapeDtypeStruct(whole.shape[1:], whole.dtype)
    return pl.pallas_call(
        finish_kernel,
        out_shape=[one] * 3 + [jax.ShapeDtypeStruct(x.shape, x.dtype) for x in like],
        in_specs=[vmem] * 5,
        out_specs=[hbm] * 9,
        scratch_shapes=[pltpu.SemaphoreType.DMA((6 * N + 6,))],
        compiler_params=pltpu.CompilerParams(vmem_limit_bytes=FINISH_LIMIT),
        cost_estimate=pl.CostEstimate(flops=10**8, bytes_accessed=100 * 2**20, transcendentals=0),
        name="finish",
    )(*moments, whole)


def wide_tiles(t, *major):
    rows = t.shape[-2] // functools.reduce(lambda a, b: a * b, major, 1)
    lead = t.shape[:-2]
    t = t.reshape(*lead, *major, rows, t.shape[-1] // 128, 128)
    return jnp.swapaxes(t, -3, -2)


def tall_tiles(t, *major):
    rows = t.shape[-2] // functools.reduce(lambda a, b: a * b, major, 1)
    lead = t.shape[:-2]
    t = t.reshape(*lead, *major, rows // 8, 8, t.shape[-1] // 128, 128)
    t = jnp.swapaxes(t, -3, -2)
    return t.reshape(*lead, *major, -1, 8, 128)


def from_wide(t, shape):
    return jnp.swapaxes(t, -3, -2).reshape(shape)


def from_tall(t, shape):
    columns = shape[-1] // 128
    t = t.reshape(*t.shape[:-3], t.shape[-3] // columns, columns, 8, 128)
    return jnp.swapaxes(t, -3, -2).reshape(shape)


def solution(mesh):
    def step(*arrays):
        terms, weights, m, v = (arrays[i : i + 3] for i in (0, 3, 6, 9))
        g = [wide_tiles(terms[0][0], N, N, N), wide_tiles(terms[1][0], N, N, N), tall_tiles(terms[2][0], N, N, N)]
        w = [wide_tiles(weights[0], N, N, N), wide_tiles(weights[1], N, N, N), tall_tiles(weights[2], N, N, N)]
        tiles = g[0].shape[4]

        def moments(one):
            return wide_tiles(one[0]), wide_tiles(one[1]), tall_tiles(one[2])

        m, v = moments(m), moments(v)
        *new_moments, whole = device_step(g, w, m, v, tiles)
        new = finish(new_moments, whole, (*m, *v))
        shapes = [one.shape for one in arrays[3:]]
        return tuple((from_tall if i % 3 == 2 else from_wide)(one, shape) for i, (one, shape) in enumerate(zip(new, shapes, strict=True)))

    all_of, cut = P(None, None, None), P(None, "dp", None)
    return jax.shard_map(
        step,
        mesh=mesh,
        in_specs=(P(("rep", "dp"), None, None, None),) * 3 + (all_of,) * 3 + (cut,) * 6,
        out_specs=(P("rep", None, None),) * 3 + (P("rep", "dp", None),) * 6,
        check_vma=False,
    )
```
